128 devices in a mesh: row: 8 (over y, core), col: 16 (over z, x).
Axes of the slice: x: 4, y: 4, z: 4, core: 2. Of those that a mesh axis runs over, the one named last changes fastest.
Arguments:
- factors: bfloat16 [128, 2, 512, 512], P(('row', 'col')), as said below
- target: int32 [256, 1], P(('row', 'col')), may hold values from 0 to 127; in each aligned block of 256 rows (0 to 255, 256 to 511, ...) at most 3 rows name the same one
Outputs:
- roots: float32 [128, 3, 512, 512], P(('row', 'col'))
The draws below stay inside these ranges and needn't reach their ends.
Inputs may be any that keep to these rules, and one draw needn't show every extreme that they name: `factors`: every block is symmetric and positive definite. `target`: every device receives between 1 and 3 blocks; some device receives exactly 3.
All inputs are finite; a program needn't handle non-finite values.
Results may differ from the reference program's by a relative error of at most 0.0003.
Values may be sent and summed in bfloat16 or wider, within the bound.
A program may use at most 128 MiB of HBM per device.

```python
import math
import jax
import jax.numpy as jnp
import numpy as np
from jax import lax

BW = 512
HOLD = 2
ITERS = 3
CAP = 3
N_ROW = 8
N_COL = 16


def draw_factors(key, part):
    key_noise, key_diag, key_scale = jax.random.split(key, 3)
    block_total = N_ROW * N_COL * HOLD
    noise = jax.random.normal(key_noise, (block_total, BW, BW), jnp.float32)
    diagonal = jnp.exp(jax.random.uniform(key_diag, (block_total, BW), jnp.float32, 0.0, math.log(10.0)))
    symmetric = (noise + jnp.swapaxes(noise, 1, 2)) / math.sqrt(2.0)
    inner = jnp.eye(BW, dtype=jnp.float32)[None] + 0.4 / math.sqrt(BW) * symmetric
    half_diag = jnp.sqrt(diagonal)
    blocks = half_diag[:, :, None] * inner * half_diag[:, None, :]
    column = jnp.arange(block_total) // HOLD % N_COL
    rising = 1.0 + 2.0 * column.astype(jnp.float32) / max(N_COL - 1, 1)
    jitter = jnp.exp(jax.random.uniform(key_scale, (block_total,), jnp.float32, math.log(0.8), math.log(1.25)))
    blocks = blocks * (rising * jitter)[:, None, None]
    return blocks.reshape(N_ROW * N_COL, HOLD, BW, BW).astype(jnp.bfloat16)


def assign_block(own_key, own, number, rows, count, top, reach, slope):
    order = jax.random.permutation(own_key, count)
    heavy_load, common = shares(count, rows * top, reach, slope, True), shares(count, rows * top, reach, slope, False)
    places = jnp.arange(count)

    def named(tallies, rotation):
        used = int((tallies > 0).sum())
        fixed = max(1, used // 4)
        moved = fixed + (places - fixed + rotation * (used - fixed)) % max(1, count - fixed)
        return jnp.zeros((count,), jnp.int32).at[order[jnp.where(places < fixed, places, moved)]].set(jnp.asarray(tallies, jnp.int32))

    tallies = jnp.where(number % 4 == 0, named(heavy_load, number // 4), named(common, number - number // 4 - 1))
    mixed = jax.random.permutation(jax.random.fold_in(own, 3), count)
    giver, sink = mixed[0:count // 2 * 2:2], mixed[1:count // 2 * 2:2]
    room = jnp.minimum(tallies[giver] - 1, reach - tallies[sink]) // 2
    room = jnp.where((giver == order[0]) | (sink == order[0]) | (tallies[sink] == 0), 0, jnp.maximum(room, 0))
    moved = jax.random.randint(jax.random.fold_in(own, 4), (count // 2,), 0, 1 << 20) % (room + 1)
    tallies = tallies.at[giver].add(-moved).at[sink].add(moved)
    items = jnp.searchsorted(jnp.cumsum(tallies), jnp.arange(rows * top), side="right").astype(jnp.int32)
    listing = items.reshape(top, rows).T
    listing = listing[jax.random.permutation(jax.random.fold_in(own, 1), rows)]
    rotation = jax.random.randint(jax.random.fold_in(own, 2), (rows, 1), 0, top)
    return jnp.take_along_axis(listing, (jnp.arange(top)[None, :] + rotation) % top, axis=1)


def shares(count, total, limit, slope, full):
    loads = [(1 << 20) // math.isqrt(rank ** slope) + 1 for rank in range(1, count + 1)]
    largest = limit if full else min(limit, max(-(-total // count), total * loads[0] // sum(loads)))
    least = 1 if total - largest >= count - 1 else 0
    counts, surplus = [largest] + [least] * (count - 1), total - largest - least * (count - 1)
    while surplus > 0:
        candidates = [i for i in range(1, count) if counts[i] < largest] or [i for i in range(1, count) if counts[i] < limit]
        pool, remaining = sum([loads[i] for i in candidates]), surplus
        for i in candidates:
            more = min(limit - counts[i], max(1, remaining * loads[i] // pool), surplus)
            counts[i] = counts[i] + more
            surplus = surplus - more
    return np.array(counts)


def setup_inputs(seed: int = 0) -> dict:
    key_list = jax.random.split(jax.random.key(seed), 3)
    factors = draw_factors(jax.random.fold_in(key_list[2], 71), 0)
    target_keys = jax.random.split(jax.random.fold_in(key_list[1], 1), (N_ROW * N_COL * HOLD) // (N_ROW * N_COL * HOLD))
    target_turns = jax.random.permutation(jax.random.fold_in(key_list[1], 3), (N_ROW * N_COL * HOLD) // (N_ROW * N_COL * HOLD))
    target = jax.vmap(lambda own, number: assign_block(jax.random.fold_in(key_list[1], 2), own, number, N_ROW * N_COL * HOLD, N_ROW * N_COL, 1, CAP, 2))(target_keys, target_turns).reshape((N_ROW * N_COL * HOLD, 1))
    return dict(factors=factors, target=target)


HIGH = lax.Precision.HIGHEST

def newton_root(block, scale):
    identity = jnp.eye(BW, dtype=jnp.float32)
    moment = block / scale
    root_iter = identity
    for repeat in range(ITERS):
        step_mat = 1.25 * identity - 0.25 * moment
        square_mat = jnp.dot(step_mat, step_mat, precision=HIGH)
        fourth_mat = jnp.dot(square_mat, square_mat, precision=HIGH)
        moment = jnp.dot(fourth_mat, moment, precision=HIGH)
        root_iter = jnp.dot(root_iter, step_mat, precision=HIGH)
    return root_iter * scale ** (-0.25)

def reference(factors, target):
    block_total = N_ROW * N_COL * HOLD
    blocks = factors.reshape(block_total, BW, BW).astype(jnp.float32)
    block_sq = lax.optimization_barrier(jnp.sum(blocks * blocks, axis=(1, 2)))
    source_rows = jnp.arange(block_total, dtype=jnp.int32) // (N_COL * HOLD)
    layer_totals = lax.optimization_barrier(jnp.sum(block_sq.reshape(N_ROW, N_COL * HOLD), axis=1))
    scales = 2.0 * jnp.sqrt(layer_totals[source_rows] / (N_COL * HOLD * BW))
    results = lax.map(lambda operands: newton_root(operands[0], operands[1]), (blocks, scales))
    targets = target[:, 0].astype(jnp.int32)
    peer_ids = jnp.arange(N_ROW * N_COL, dtype=jnp.int32)
    matches = (targets[:, None] == peer_ids[None, :]).astype(jnp.int32)
    slot_index = lax.optimization_barrier(jnp.sum((jnp.cumsum(matches, axis=0) - matches) * matches, axis=1)).astype(jnp.int32)
    output = jnp.zeros((N_ROW * N_COL, CAP, BW, BW), jnp.float32)
    return output.at[targets, slot_index].set(results)
```

```python
import functools

import jax
import jax.numpy as jnp
from jax import lax
from jax.experimental import pallas as pl
from jax.experimental.pallas import tpu as pltpu
from jax.sharding import Mesh
from jax.sharding import PartitionSpec as P

AXES = ("y", "c", "z", "x")
MESH = pl.DeviceIdType.MESH
DEVICES = 128
HALF = 256
CAP = 3
F32 = jnp.float32
BF16 = jnp.bfloat16


def iota(shape, dim):
    return lax.broadcasted_iota(jnp.int32, shape, dim)


def total(value):
    return jnp.sum(jnp.sum(value, axis=1, keepdims=True), axis=0, keepdims=True)


def peer(k, here):
    y, c, z, x = here
    k = (k * 37) & (DEVICES - 1)
    there = (
        (y + ((k >> 4) & 3)) & 3,
        (c + (k >> 6)) & 1,
        (z + ((k >> 2) & 3)) & 3,
        (x + (k & 3)) & 3,
    )
    return there, ((there[0] * 2 + there[1]) * 4 + there[2]) * 4 + there[3]


def pack(f_ref, t_ref, send1, meta):
    row, col = iota((HALF, HALF), 0), iota((HALF, HALF), 1)
    sq = jnp.zeros((1, 1), F32)
    diagonals = []
    for h in range(2):
        a = f_ref[h, 0:HALF, 0:HALF].astype(F32)
        b = f_ref[h, 0:HALF, HALF:]
        c = f_ref[h, HALF:, 0:HALF].astype(F32)
        d = f_ref[h, HALF:, HALF:].astype(F32)
        bf = b.astype(F32)
        sq = sq + total(a * a + bf * bf + c * c + d * d)
        v = jnp.where(row <= col, a, d).astype(BF16)
        diagonals.append(jnp.sum(jnp.where(row == col, d, 0.0), axis=0, keepdims=True))
        for part, w in enumerate((b, v)):
            for lanes in range(2):
                start = lanes * 64 + part * 32
                piece = w[:, lanes * 128 : lanes * 128 + 128]
                send1[h, start : start + 32] = piece.reshape(32, 8, 128)
    high = sq.astype(BF16).astype(F32)
    middle = (sq - high).astype(BF16).astype(F32)
    low = sq - high - middle
    line, lane = iota((8, 128), 0), iota((8, 128), 1)
    facts = jnp.zeros((8, 128), F32)
    words = (t_ref[0, 0].astype(F32), t_ref[1, 0].astype(F32), high, middle, low)
    for at, word in enumerate(words):
        facts = jnp.where(lane == at, word, facts)
    out = jnp.where(line == 4, facts, 0.0)
    for h in range(2):
        for lanes in range(2):
            piece = diagonals[h][:, lanes * 128 : lanes * 128 + 128]
            out = jnp.where(line == 2 * h + lanes, piece, out)
    meta[...] = out.astype(BF16)


def plan(me, all_meta, order, aux_ref):
    table = all_meta[...].reshape(DEVICES * 8, 128)
    pick = iota((DEVICES, DEVICES * 8), 1) == iota((DEVICES, DEVICES * 8), 0) * 8 + 4
    facts = jnp.dot(
        jnp.where(pick, 1.0, 0.0).astype(BF16), table, preferred_element_type=F32
    )
    across = facts.T
    t0, t1 = facts[:, 0:1], facts[:, 1:2]
    r0, r1 = across[0:1, :], across[1:2, :]
    sq = (across[2:3, :] + across[3:4, :]) + across[4:5, :]
    i, j = iota((DEVICES, DEVICES), 0), iota((DEVICES, DEVICES), 1)

    def same(a, b):
        return jnp.where(a == b, 1.0, 0.0)

    def along(value):
        return jnp.sum(value, axis=1, keepdims=True)

    before = j < i
    slot0 = along(jnp.where(before, same(r0, t0) + same(r1, t0), 0.0))
    slot1 = along(jnp.where(before, same(r0, t1) + same(r1, t1), 0.0)) + same(t0, t1)
    layer = along(jnp.where((i >> 4) == (j >> 4), sq, 0.0))
    fi, fj = i.astype(F32), j.astype(F32)
    line, lane = iota((8, 128), 0), iota((8, 128), 1)
    mine = iota((1, 128), 1) == me
    wanted = jnp.zeros((8, 128), F32)
    spots = jnp.full((8, 1), -1.0, F32)
    numbers = jnp.zeros((8, 128), F32)
    for s in range(CAP):
        first = jnp.where(t0 == fj, same(slot0, s), 0.0)
        second = jnp.where(t1 == fj, same(slot1, s), 0.0)
        both = first + second
        holds = jnp.sum(first * fi + second * (fi + DEVICES), axis=0, keepdims=True)
        filled = jnp.sum(both, axis=0, keepdims=True)
        layers = jnp.sum(both * layer, axis=0, keepdims=True)
        wanted = jnp.where(line == s, holds, wanted)
        my_block = along(jnp.where(mine, holds, 0.0))
        my_filled = along(jnp.where(mine, filled, 0.0))
        my_layer = along(jnp.where(mine, layers, 0.0))
        scale = 2.0 * jnp.sqrt(jnp.where(my_filled > 0, my_layer, 16384.0) / 16384.0)
        inverse = jnp.where(my_filled > 0, 1.0 / scale, 0.0)
        factor = jnp.where(my_filled > 0, lax.rsqrt(jnp.sqrt(scale)), 0.0)
        numbers = jnp.where((line == s) & (lane == 0), inverse, numbers)
        numbers = jnp.where((line == s) & (lane == 1), factor, numbers)
        late = jnp.where(my_block >= DEVICES, 1.0, 0.0)
        spot = (my_block - late * DEVICES) * 8.0 + late * 2.0
        for lanes in range(2):
            spots = jnp.where(iota((8, 1), 0) == 2 * s + lanes, spot + lanes, spots)
    order[...] = wanted.astype(jnp.int32)
    pick = iota((8, DEVICES * 8), 1).astype(F32) == spots
    aux_ref[0:8, :] = jnp.dot(
        jnp.where(pick, 1.0, 0.0).astype(BF16), table, preferred_element_type=F32
    )
    aux_ref[8:16, :] = numbers


def move_kernel(
    f_ref, t_ref, g_ref, aux_ref,
    send1, got1, meta, all_meta, send2, got2, order, order_s,
    meta_out, meta_in, out1, in1, out2, in2, local,
):
    here = tuple(lax.axis_index(a) for a in AXES)
    me = ((here[0] * 2 + here[1]) * 4 + here[2]) * 4 + here[3]
    barrier = pltpu.get_barrier_semaphore()

    @pl.loop(1, DEVICES)
    def _(k):
        there, _ = peer(k, here)
        pl.semaphore_signal(barrier, 1, device_id=there, device_id_type=MESH)

    pack(f_ref, t_ref, send1, meta)
    pl.semaphore_wait(barrier, DEVICES - 1)

    @pl.loop(1, DEVICES)
    def _(k):
        there, _ = peer(k, here)
        pltpu.make_async_remote_copy(
            src_ref=meta, dst_ref=all_meta.at[me], send_sem=meta_out, recv_sem=meta_in,
            device_id=there, device_id_type=MESH,
        ).start()

    @pl.loop(1, DEVICES)
    def _(k):
        there, index = peer(k, here)
        pltpu.make_async_remote_copy(
            src_ref=send1.at[:, index], dst_ref=got1.at[:, me], send_sem=out1, recv_sem=in1,
            device_id=there, device_id_type=MESH,
        ).start()

    all_meta[me] = meta[...]
    got1[:, me] = send1[:, me]

    def settle(buffer, *sems):
        for sem in sems:
            pltpu.make_async_copy(buffer, buffer, sem).wait()

    settle(all_meta.at[0 : DEVICES - 1], meta_in, meta_out)
    plan(me, all_meta, order, aux_ref)
    copy = pltpu.make_async_copy(order, order_s, local)
    copy.start()
    copy.wait()
    settle(got1.at[:, 0 : DEVICES - 1], in1, out1)
    for s in range(CAP):

        @pl.loop(0, DEVICES, unroll=8)
        def _(d, s=s):
            block = order_s[s, d]
            send2[s, d] = got1[(block >> 7) & 1, block & (DEVICES - 1)]

        @pl.loop(1, DEVICES)
        def _(k, s=s):
            there, index = peer(k, here)
            pltpu.make_async_remote_copy(
                src_ref=send2.at[s, index], dst_ref=got2.at[s, me], send_sem=out2.at[s], recv_sem=in2.at[s],
                device_id=there, device_id_type=MESH,
            ).start()

        got2[s, me] = send2[s, me]
    for s in range(CAP):
        settle(got2.at[s, 0 : DEVICES - 1], in2.at[s], out2.at[s])
        g_ref[s] = got2[s]


def move(factors, target):
    vmem, dma = pltpu.VMEM, pltpu.SemaphoreType.DMA
    return pl.pallas_call(
        move_kernel,
        out_shape=(
            jax.ShapeDtypeStruct((CAP, DEVICES, 8, 128), BF16),
            jax.ShapeDtypeStruct((16, 128), F32),
        ),
        in_specs=[pl.BlockSpec(memory_space=vmem), pl.BlockSpec(memory_space=pltpu.SMEM)],
        out_specs=[pl.BlockSpec(memory_space=vmem)] * 2,
        scratch_shapes=[
            vmem((2, DEVICES, 8, 128), BF16),
            vmem((2, DEVICES, 8, 128), BF16),
            vmem((8, 128), BF16),
            vmem((DEVICES, 8, 128), BF16),
            vmem((CAP, DEVICES, 8, 128), BF16),
            vmem((CAP, DEVICES, 8, 128), BF16),
            vmem((8, 128), jnp.int32),
            pltpu.SMEM((8, 128), jnp.int32),
            dma, dma, dma, dma, dma((CAP,)), dma((CAP,)), dma,
        ],
        compiler_params=pltpu.CompilerParams(collective_id=0, has_side_effects=True),
        name="move",
    )(factors, target)


def split(value):
    high = value.astype(BF16)
    return high, (value - high.astype(F32)).astype(BF16)


def dot(a, b):
    return jnp.dot(a, b, preferred_element_type=F32)


def product(left, right):
    return dot(left[0], right[0]) + (dot(left[0], right[1]) + dot(left[1], right[0]))


def root_kernel(g_ref, aux_ref, o_ref, block):
    s = pl.program_id(0)
    row, col = iota((HALF, HALF), 0), iota((HALF, HALF), 1)

    def whole(part):
        return jnp.concatenate(
            [
                g_ref[0, lanes * 64 + part * 32 : lanes * 64 + part * 32 + 32].reshape(HALF, 128)
                for lanes in range(2)
            ],
            axis=1,
        )

    u = whole(0)
    v = whole(1).astype(F32)
    flipped = v.T
    diagonal = jnp.concatenate(
        [aux_ref[pl.ds(2 * s, 1), :], aux_ref[pl.ds(2 * s + 1, 1), :]], axis=1
    )
    block[0:HALF, 0:HALF] = jnp.where(row <= col, v, flipped).astype(BF16)
    block[0:HALF, HALF:] = u
    block[HALF:, 0:HALF] = u.astype(F32).T.astype(BF16)
    corner = jnp.where(row > col, v, jnp.where(row == col, diagonal, flipped))
    block[HALF:, HALF:] = corner.astype(BF16)
    inverse = aux_ref[pl.ds(8 + s, 1), 0:1]
    factor = aux_ref[pl.ds(8 + s, 1), 1:2]
    eye = jnp.where(iota((512, 512), 0) == iota((512, 512), 1), 1.25, 0.0)

    a = block[...]
    q = inverse * 0.25
    af = a.astype(F32)
    square = (1.25 * eye - (2.5 * q) * af) + (dot(a, a) * q) * q
    square = split(square)
    fifth = split((dot(square[0], a) + dot(square[1], a)) * q)
    step = eye - product(square, fifth)
    parts = split(step)
    square = product(parts, parts)
    rest = split(1.25 * step - square)
    square = split(square)
    rest = split(product(square, rest))
    both = 1.25 * step - product(square, rest)
    parts = split(both)
    out = 1.25 * both - (dot(parts[0], a) + dot(parts[1], a)) * q
    o_ref[0] = out * factor


def roots(moved, aux):
    return pl.pallas_call(
        root_kernel,
        grid=(CAP,),
        out_shape=jax.ShapeDtypeStruct((CAP, 512, 512), F32),
        in_specs=[
            pl.BlockSpec((1, DEVICES, 8, 128), lambda s: (s, 0, 0, 0)),
            pl.BlockSpec((16, 128), lambda s: (0, 0)),
        ],
        out_specs=pl.BlockSpec((1, 512, 512), lambda s: (s, 0, 0)),
        scratch_shapes=[pltpu.VMEM((512, 512), BF16)],
        name="roots",
    )(moved, aux)


def shards(factors, target):
    moved, aux = move(factors[0], target)
    return roots(moved, aux)[None]


def solution(mesh):
    finer = Mesh(mesh.devices.reshape(4, 2, 4, 4), AXES)
    placed = (P(AXES, None, None, None), P(AXES, None))
    return jax.shard_map(
        shards, mesh=finer, in_specs=placed, out_specs=P(AXES, None, None, None), check_vma=False
    )
```

```python
import functools

import jax
import jax.numpy as jnp
from jax import lax
from jax.experimental import pallas as pl
from jax.experimental.pallas import tpu as pltpu
from jax.sharding import Mesh
from jax.sharding import PartitionSpec as P

AXES = ("y", "c", "z", "x")
MESH = pl.DeviceIdType.MESH
DEVICES = 128
HALF = 256
CAP = 3
F32 = jnp.float32
BF16 = jnp.bfloat16


def iota(shape, dim):
    return lax.broadcasted_iota(jnp.int32, shape, dim)


def total(value):
    return jnp.sum(jnp.sum(value, axis=1, keepdims=True), axis=0, keepdims=True)


def peer(k, here):
    y, c, z, x = here
    k = (k * 37) & (DEVICES - 1)
    there = (
        (y + ((k >> 4) & 3)) & 3,
        (c + (k >> 6)) & 1,
        (z + ((k >> 2) & 3)) & 3,
        (x + (k & 3)) & 3,
    )
    return there, ((there[0] * 2 + there[1]) * 4 + there[2]) * 4 + there[3]


def each_peer(here, do):
    for start, stop, unroll in ((1, 8, 7), (8, DEVICES, 8)):

        @pl.loop(start, stop, unroll=unroll)
        def _(k):
            do(*peer(k, here))


def pack(f_ref, t_ref, send1, facts_ref, diagonal_ref):
    row, col = iota((HALF, HALF), 0), iota((HALF, HALF), 1)
    sq = jnp.zeros((1, 1), F32)
    line = iota((2, 128), 0)
    for h in range(2):
        a = f_ref[h, 0:HALF, 0:HALF].astype(F32)
        b = f_ref[h, 0:HALF, HALF:]
        c = f_ref[h, HALF:, 0:HALF].astype(F32)
        d = f_ref[h, HALF:, HALF:].astype(F32)
        bf = b.astype(F32)
        sq = sq + total(a * a + bf * bf + c * c + d * d)
        v = jnp.where(row <= col, a, d).astype(BF16)
        diagonal = jnp.sum(jnp.where(row == col, d, 0.0), axis=0, keepdims=True)
        diagonal = jnp.where(line == 0, diagonal[:, 0:128], diagonal[:, 128:])
        diagonal_ref[h] = diagonal.astype(BF16)
        for part, w in enumerate((b, v)):
            for lanes in range(2):
                start = lanes * 64 + part * 32
                piece = w[:, lanes * 128 : lanes * 128 + 128]
                send1[h, start : start + 32] = piece.reshape(32, 8, 128)
    lane = iota((1, 128), 1)
    facts = jnp.where(lane == 0, t_ref[0:1, 0:1].astype(F32), 0.0)
    facts = jnp.where(lane == 1, t_ref[1:2, 0:1].astype(F32), facts)
    facts_ref[...] = jnp.where(lane == 2, sq, facts)


def plan(me, all_facts, order, aux_ref):
    facts = all_facts[:, 0, :]
    across = facts.T
    t0, t1 = facts[:, 0:1], facts[:, 1:2]
    r0, r1, sq = across[0:1, :], across[1:2, :], across[2:3, :]
    i, j = iota((DEVICES, DEVICES), 0), iota((DEVICES, DEVICES), 1)

    def same(a, b):
        return jnp.where(a == b, 1.0, 0.0)

    def along(value):
        return jnp.sum(value, axis=1, keepdims=True)

    before = j < i
    slot0 = along(jnp.where(before, same(r0, t0) + same(r1, t0), 0.0))
    slot1 = along(jnp.where(before, same(r0, t1) + same(r1, t1), 0.0)) + same(t0, t1)
    layer = along(jnp.where((i >> 4) == (j >> 4), sq, 0.0))
    fi, fj = i.astype(F32), j.astype(F32)
    line, lane = iota((8, 128), 0), iota((8, 128), 1)
    mine = iota((1, 128), 1) == me
    wanted = jnp.zeros((8, 128), F32)
    numbers = jnp.zeros((8, 128), F32)
    for s in range(CAP):
        first = jnp.where(t0 == fj, same(slot0, s), 0.0)
        second = jnp.where(t1 == fj, same(slot1, s), 0.0)
        both = first + second
        holds = jnp.sum(first * fi + second * (fi + DEVICES), axis=0, keepdims=True)
        filled = jnp.sum(both, axis=0, keepdims=True)
        layers = jnp.sum(both * layer, axis=0, keepdims=True)
        wanted = jnp.where(line == s, holds, wanted)
        my_filled = along(jnp.where(mine, filled, 0.0))
        my_layer = along(jnp.where(mine, layers, 0.0))
        scale = 2.0 * jnp.sqrt(jnp.where(my_filled > 0, my_layer, 16384.0) / 16384.0)
        inverse = jnp.where(my_filled > 0, 1.0 / scale, 0.0)
        factor = jnp.where(my_filled > 0, lax.rsqrt(jnp.sqrt(scale)), 0.0)
        numbers = jnp.where((line == s) & (lane == 0), inverse, numbers)
        numbers = jnp.where((line == s) & (lane == 1), factor, numbers)
    order[...] = wanted.astype(jnp.int32)
    aux_ref[8:16, :] = numbers


def move_kernel(
    f_any, t_ref, g_ref, aux_ref,
    f_ref, send1, got1, facts, all_facts, diagonal, all_diagonal, send2, got2, order, order_s,
    facts_out, facts_in, diagonal_out, diagonal_in, out1, in1, out2, in2, local,
):
    here = tuple(lax.axis_index(a) for a in AXES)
    me = ((here[0] * 2 + here[1]) * 4 + here[2]) * 4 + here[3]
    load = pltpu.make_async_copy(f_any, f_ref, local)
    load.start()
    barrier = pltpu.get_barrier_semaphore()
    each_peer(
        here,
        lambda there, _: pl.semaphore_signal(barrier, 1, device_id=there, device_id_type=MESH),
    )
    load.wait()
    pack(f_ref, t_ref, send1, facts, diagonal)
    pl.semaphore_wait(barrier, DEVICES - 1)

    def send(source, target, gone, came):
        def start(there, index):
            pltpu.make_async_remote_copy(
                src_ref=source(index), dst_ref=target, send_sem=gone, recv_sem=came,
                device_id=there, device_id_type=MESH,
            ).start()

        each_peer(here, start)

    def settle(buffer, *sems):
        for sem in sems:
            pltpu.make_async_copy(buffer, buffer, sem).wait()

    send(lambda index: facts, all_facts.at[me], facts_out, facts_in)
    send(lambda index: send1.at[:, index], got1.at[:, me], out1, in1)
    send(lambda index: diagonal, all_diagonal.at[:, me], diagonal_out, diagonal_in)
    all_facts[me] = facts[...]
    got1[:, me] = send1[:, me]
    all_diagonal[:, me] = diagonal[...]
    settle(all_facts.at[0 : DEVICES - 1], facts_in, facts_out)
    plan(me, all_facts, order, aux_ref)
    copy = pltpu.make_async_copy(order, order_s, local)
    copy.start()
    copy.wait()
    settle(got1.at[:, 0 : DEVICES - 1], in1, out1)

    def place(block):
        return (block >> 7) & 1, block & (DEVICES - 1)

    for s in range(CAP):

        @pl.loop(0, DEVICES, unroll=8)
        def _(d, s=s):
            send2[s, d] = got1[place(order_s[s, d])]

        send(lambda index, s=s: send2.at[s, index], got2.at[s, me], out2.at[s], in2.at[s])
        got2[s, me] = send2[s, me]
    settle(all_diagonal.at[:, 0 : DEVICES - 1], diagonal_in, diagonal_out)
    for s in range(CAP):
        aux_ref[2 * s : 2 * s + 2, :] = all_diagonal[place(order_s[s, me])].astype(F32)
        settle(got2.at[s, 0 : DEVICES - 1], in2.at[s], out2.at[s])
        g_ref[s] = got2[s]


def move(factors, target):
    vmem, dma = pltpu.VMEM, pltpu.SemaphoreType.DMA
    return pl.pallas_call(
        move_kernel,
        out_shape=(
            jax.ShapeDtypeStruct((CAP, DEVICES, 8, 128), BF16),
            jax.ShapeDtypeStruct((16, 128), F32),
        ),
        in_specs=[pl.BlockSpec(memory_space=pl.ANY), pl.BlockSpec(memory_space=vmem)],
        out_specs=[pl.BlockSpec(memory_space=vmem)] * 2,
        scratch_shapes=[
            vmem((2, 512, 512), BF16),
            vmem((2, DEVICES, 8, 128), BF16),
            vmem((2, DEVICES, 8, 128), BF16),
            vmem((1, 128), F32),
            vmem((DEVICES, 1, 128), F32),
            vmem((2, 2, 128), BF16),
            vmem((2, DEVICES, 2, 128), BF16),
            vmem((CAP, DEVICES, 8, 128), BF16),
            vmem((CAP, DEVICES, 8, 128), BF16),
            vmem((8, 128), jnp.int32),
            pltpu.SMEM((8, 128), jnp.int32),
            dma, dma, dma, dma, dma, dma, dma((CAP,)), dma((CAP,)), dma,
        ],
        compiler_params=pltpu.CompilerParams(collective_id=0, has_side_effects=True),
        name="move",
    )(factors, target)


def dot(a, b):
    return jnp.dot(a, b, preferred_element_type=F32)


LEFT, RIGHT = slice(0, HALF), slice(HALF, 2 * HALF)


def tiles(ref):
    return [ref[r, c].astype(F32) for r, c in ((LEFT, LEFT), (LEFT, RIGHT), (RIGHT, RIGHT))]


def product(*pairs):
    right = sum(dot(a[...], b[:, RIGHT]) for a, b in pairs)
    corner = sum(dot(a[LEFT, :], b[:, LEFT]) for a, b in pairs)
    return [corner, right[LEFT], right[RIGHT]]


def times(a, b):
    return product((a[0], b[0]), (a[0], b[1]), (a[1], b[0]))


def keep(ref, value):
    places = (LEFT, LEFT), (LEFT, RIGHT), (RIGHT, RIGHT), (RIGHT, LEFT)
    for (r, c), tile in zip(places, (*value, value[1].T)):
        high = tile.astype(BF16)
        ref[0, r, c] = high
        ref[1, r, c] = (tile - high.astype(F32)).astype(BF16)


def unfold(g, diagonal, block):
    row, col = iota((HALF, HALF), 0), iota((HALF, HALF), 1)

    def whole(part):
        return jnp.concatenate(
            [
                g[lanes * 64 + part * 32 : lanes * 64 + part * 32 + 32].reshape(HALF, 128)
                for lanes in range(2)
            ],
            axis=1,
        )

    u = whole(0)
    v = whole(1).astype(F32)
    flipped = v.T
    block[LEFT, LEFT] = jnp.where(row <= col, v, flipped).astype(BF16)
    block[LEFT, RIGHT] = u
    block[RIGHT, LEFT] = u.astype(F32).T.astype(BF16)
    corner = jnp.where(row > col, v, jnp.where(row == col, diagonal, flipped))
    block[RIGHT, RIGHT] = corner.astype(BF16)


def newton(block, inverse, factor, out, x, y, z):
    eye = jnp.where(iota((HALF, HALF), 0) == iota((HALF, HALF), 1), 1.25, 0.0)
    eyes = (eye, 0.0, eye)
    q = inverse * 0.25
    square = product((block, block))
    keep(x, [1.25 * e - (2.5 * q) * a + (s * q) * q for e, a, s in zip(eyes, tiles(block), square)])
    keep(y, [t * q for t in product((x.at[0], block), (x.at[1], block))])
    step = [e - t for e, t in zip(eyes, times(x, y))]
    keep(z, step)
    square = times(z, z)
    keep(x, square)
    keep(y, [1.25 * t - s for t, s in zip(step, square)])
    keep(z, times(x, y))
    both = [1.25 * t - f for t, f in zip(step, times(x, z))]
    keep(y, both)
    rest = product((y.at[0], block), (y.at[1], block))
    root = [(1.25 * t - r * q) * factor for t, r in zip(both, rest)]
    out[LEFT, LEFT] = root[0]
    out[LEFT, RIGHT] = root[1]
    out[RIGHT, RIGHT] = root[2]
    out[RIGHT, LEFT] = root[1].T


def root_kernel(g_ref, aux_ref, o_ref, block, x, y, z):
    s = pl.program_id(0)
    diagonal = jnp.concatenate(
        [aux_ref[pl.ds(2 * s, 1), :], aux_ref[pl.ds(2 * s + 1, 1), :]], axis=1
    )
    unfold(g_ref.at[0], diagonal, block)
    inverse = aux_ref[pl.ds(8 + s, 1), 0:1]
    factor = aux_ref[pl.ds(8 + s, 1), 1:2]
    newton(block, inverse, factor, o_ref.at[0], x, y, z)


def roots(moved, aux):
    return pl.pallas_call(
        root_kernel,
        grid=(CAP,),
        out_shape=jax.ShapeDtypeStruct((CAP, 512, 512), F32),
        in_specs=[
            pl.BlockSpec((1, DEVICES, 8, 128), lambda s: (s, 0, 0, 0)),
            pl.BlockSpec((16, 128), lambda s: (0, 0)),
        ],
        out_specs=pl.BlockSpec((1, 512, 512), lambda s: (s, 0, 0)),
        scratch_shapes=[pltpu.VMEM((512, 512), BF16)] + [pltpu.VMEM((2, 512, 512), BF16)] * 3,
        name="roots",
    )(moved, aux)


def shards(factors, target):
    moved, aux = move(factors[0], target)
    return roots(moved, aux)[None]


def solution(mesh):
    finer = Mesh(mesh.devices.reshape(4, 2, 4, 4), AXES)
    placed = (P(AXES, None, None, None), P(AXES, None))
    return jax.shard_map(
        shards, mesh=finer, in_specs=placed, out_specs=P(AXES, None, None, None), check_vma=False
    )
```

```python
import itertools

import jax
import jax.numpy as jnp
from jax import lax
from jax.experimental import pallas as pl
from jax.experimental.pallas import tpu as pltpu
from jax.sharding import Mesh
from jax.sharding import PartitionSpec as P

AXES = ("y", "c", "z", "x")
MESH = pl.DeviceIdType.MESH
DEVICES = 128
HALF = 256
CAP = 3
F32 = jnp.float32
BF16 = jnp.bfloat16


def iota(shape, dim):
    return lax.broadcasted_iota(jnp.int32, shape, dim)


def total(value):
    return jnp.sum(jnp.sum(value, axis=1, keepdims=True), axis=0, keepdims=True)


def peer(k, here):
    y, c, z, x = here
    k = (k * 37) & (DEVICES - 1)
    there = (
        (y + ((k >> 4) & 3)) & 3,
        (c + (k >> 6)) & 1,
        (z + ((k >> 2) & 3)) & 3,
        (x + (k & 3)) & 3,
    )
    return there, ((there[0] * 2 + there[1]) * 4 + there[2]) * 4 + there[3]


def each_peer(here, do):
    for start, stop, unroll in ((1, 8, 7), (8, DEVICES, 8)):

        @pl.loop(start, stop, unroll=unroll)
        def _(k):
            do(*peer(k, here))


def pack(f_ref, t_ref, send1, facts_ref, diagonal_ref):
    row, col = iota((HALF, HALF), 0), iota((HALF, HALF), 1)
    sq = jnp.zeros((1, 1), F32)
    line = iota((2, 128), 0)
    for h in range(2):
        a = f_ref[h, 0:HALF, 0:HALF].astype(F32)
        b = f_ref[h, 0:HALF, HALF:]
        c = f_ref[h, HALF:, 0:HALF].astype(F32)
        d = f_ref[h, HALF:, HALF:].astype(F32)
        bf = b.astype(F32)
        sq = sq + total(a * a + bf * bf + c * c + d * d)
        v = jnp.where(row <= col, a, d).astype(BF16)
        diagonal = jnp.sum(jnp.where(row == col, d, 0.0), axis=0, keepdims=True)
        diagonal = jnp.where(line == 0, diagonal[:, 0:128], diagonal[:, 128:])
        diagonal_ref[h] = diagonal.astype(BF16)
        for part, w in enumerate((b, v)):
            for lanes in range(2):
                start = lanes * 64 + part * 32
                piece = w[:, lanes * 128 : lanes * 128 + 128]
                send1[h, start : start + 32] = piece.reshape(32, 8, 128)
    lane = iota((1, 128), 1)
    facts = jnp.where(lane == 0, t_ref[0:1, 0:1].astype(F32), 0.0)
    facts = jnp.where(lane == 1, t_ref[1:2, 0:1].astype(F32), facts)
    facts_ref[...] = jnp.where(lane == 2, sq, facts)


def plan(me, all_facts, order, aux_ref):
    facts = all_facts[:, 0, :]
    across = facts.T
    t0, t1 = facts[:, 0:1], facts[:, 1:2]
    r0, r1, sq = across[0:1, :], across[1:2, :], across[2:3, :]
    i, j = iota((DEVICES, DEVICES), 0), iota((DEVICES, DEVICES), 1)

    def same(a, b):
        return jnp.where(a == b, 1.0, 0.0)

    def along(value):
        return jnp.sum(value, axis=1, keepdims=True)

    before = j < i
    slot0 = along(jnp.where(before, same(r0, t0) + same(r1, t0), 0.0))
    slot1 = along(jnp.where(before, same(r0, t1) + same(r1, t1), 0.0)) + same(t0, t1)
    layer = along(jnp.where((i >> 4) == (j >> 4), sq, 0.0))
    fi, fj = i.astype(F32), j.astype(F32)
    line, lane = iota((8, 128), 0), iota((8, 128), 1)
    mine = iota((1, 128), 1) == me
    wanted = jnp.zeros((8, 128), F32)
    numbers = jnp.zeros((8, 128), F32)
    for s in range(CAP):
        first = jnp.where(t0 == fj, same(slot0, s), 0.0)
        second = jnp.where(t1 == fj, same(slot1, s), 0.0)
        both = first + second
        holds = jnp.sum(first * fi + second * (fi + DEVICES), axis=0, keepdims=True)
        filled = jnp.sum(both, axis=0, keepdims=True)
        layers = jnp.sum(both * layer, axis=0, keepdims=True)
        wanted = jnp.where(line == s, holds, wanted)
        my_filled = along(jnp.where(mine, filled, 0.0))
        my_layer = along(jnp.where(mine, layers, 0.0))
        scale = 2.0 * jnp.sqrt(jnp.where(my_filled > 0, my_layer, 16384.0) / 16384.0)
        inverse = jnp.where(my_filled > 0, 1.0 / scale, 0.0)
        factor = jnp.where(my_filled > 0, lax.rsqrt(jnp.sqrt(scale)), 0.0)
        numbers = jnp.where((line == s) & (lane == 0), inverse, numbers)
        numbers = jnp.where((line == s) & (lane == 1), factor, numbers)
    order[...] = wanted.astype(jnp.int32)
    aux_ref[8:16, :] = numbers


def dot(a, b):
    return jnp.dot(a, b, preferred_element_type=F32)


LEFT, RIGHT = slice(0, HALF), slice(HALF, 2 * HALF)


def tiles(ref):
    return [ref[r, c].astype(F32) for r, c in ((LEFT, LEFT), (LEFT, RIGHT), (RIGHT, RIGHT))]


def product(*pairs):
    right = sum(dot(a[...], b[:, RIGHT]) for a, b in pairs)
    corner = sum(dot(a[LEFT, :], b[:, LEFT]) for a, b in pairs)
    return [corner, right[LEFT], right[RIGHT]]


def times(a, b):
    return product((a[0], b[0]), (a[0], b[1]), (a[1], b[0]))


def keep(ref, value):
    places = (LEFT, LEFT), (LEFT, RIGHT), (RIGHT, RIGHT), (RIGHT, LEFT)
    for (r, c), tile in zip(places, (*value, value[1].T)):
        high = tile.astype(BF16)
        ref[0, r, c] = high
        ref[1, r, c] = (tile - high.astype(F32)).astype(BF16)


def unfold(g, diagonal, block):
    row, col = iota((HALF, HALF), 0), iota((HALF, HALF), 1)

    def whole(part):
        return jnp.concatenate(
            [
                g[lanes * 64 + part * 32 : lanes * 64 + part * 32 + 32].reshape(HALF, 128)
                for lanes in range(2)
            ],
            axis=1,
        )

    u = whole(0)
    v = whole(1).astype(F32)
    flipped = v.T
    block[LEFT, LEFT] = jnp.where(row <= col, v, flipped).astype(BF16)
    block[LEFT, RIGHT] = u
    block[RIGHT, LEFT] = u.astype(F32).T.astype(BF16)
    corner = jnp.where(row > col, v, jnp.where(row == col, diagonal, flipped))
    block[RIGHT, RIGHT] = corner.astype(BF16)


def newton(block, inverse, factor, out, x, y, z):
    eye = jnp.where(iota((HALF, HALF), 0) == iota((HALF, HALF), 1), 1.25, 0.0)
    eyes = (eye, 0.0, eye)
    q = inverse * 0.25
    square = product((block, block))
    keep(x, [1.25 * e - (2.5 * q) * a + (s * q) * q for e, a, s in zip(eyes, tiles(block), square)])
    yield
    keep(y, [t * q for t in product((x.at[0], block), (x.at[1], block))])
    yield
    step = [e - t for e, t in zip(eyes, times(x, y))]
    keep(z, step)
    yield
    square = times(z, z)
    keep(x, square)
    keep(y, [1.25 * t - s for t, s in zip(step, square)])
    yield
    keep(z, times(x, y))
    yield
    both = [1.25 * t - f for t, f in zip(step, times(x, z))]
    keep(y, both)
    yield
    rest = product((y.at[0], block), (y.at[1], block))
    root = [(1.25 * t - r * q) * factor for t, r in zip(both, rest)]
    out[LEFT, LEFT] = root[0]
    out[LEFT, RIGHT] = root[1]
    out[RIGHT, RIGHT] = root[2]
    out[RIGHT, LEFT] = root[1].T


def begin(s, g, aux_ref, out, block, x, y, z):
    unfold(g, jnp.concatenate([aux_ref[2 * s : 2 * s + 1], aux_ref[2 * s + 1 : 2 * s + 2]], axis=1), block)
    return newton(block, aux_ref[8 + s : 9 + s, 0:1], aux_ref[8 + s : 9 + s, 1:2], out, x, y, z)


def move_kernel(
    f_any, t_ref, g_ref, aux_ref, out_any,
    f_ref, send1, got1, facts, all_facts, diagonal, all_diagonal, send2, got2, order, order_s,
    root, block, x, y, z,
    facts_out, facts_in, diagonal_out, diagonal_in, out1, in1, out2, in2, local,
):
    here = tuple(lax.axis_index(a) for a in AXES)
    me = ((here[0] * 2 + here[1]) * 4 + here[2]) * 4 + here[3]
    load = pltpu.make_async_copy(f_any, f_ref, local)
    load.start()
    barrier = pltpu.get_barrier_semaphore()
    each_peer(
        here,
        lambda there, _: pl.semaphore_signal(barrier, 1, device_id=there, device_id_type=MESH),
    )
    load.wait()
    pack(f_ref, t_ref, send1, facts, diagonal)
    pl.semaphore_wait(barrier, DEVICES - 1)

    def send(source, target, gone, came):
        def start(there, index):
            pltpu.make_async_remote_copy(
                src_ref=source(index), dst_ref=target, send_sem=gone, recv_sem=came,
                device_id=there, device_id_type=MESH,
            ).start()

        each_peer(here, start)

    def settle(buffer, *sems):
        for sem in sems:
            pltpu.make_async_copy(buffer, buffer, sem).wait()

    send(lambda index: facts, all_facts.at[me], facts_out, facts_in)
    send(lambda index: send1.at[:, index], got1.at[:, me], out1, in1)
    send(lambda index: diagonal, all_diagonal.at[:, me], diagonal_out, diagonal_in)
    all_facts[me] = facts[...]
    got1[:, me] = send1[:, me]
    all_diagonal[:, me] = diagonal[...]
    settle(all_facts.at[0 : DEVICES - 1], facts_in, facts_out)
    plan(me, all_facts, order, aux_ref)
    copy = pltpu.make_async_copy(order, order_s, local)
    copy.start()
    copy.wait()
    settle(got1.at[:, 0 : DEVICES - 1], in1, out1)

    def place(block):
        return (block >> 7) & 1, block & (DEVICES - 1)

    for s in range(CAP):

        @pl.loop(0, DEVICES, unroll=8)
        def _(d, s=s):
            send2[s, d] = got1[place(order_s[s, d])]

        send(lambda index, s=s: send2.at[s, index], got2.at[s, me], out2.at[s], in2.at[s])
        got2[s, me] = send2[s, me]
    settle(all_diagonal.at[:, 0 : DEVICES - 1], diagonal_in, diagonal_out)
    for s in range(CAP):
        aux_ref[2 * s : 2 * s + 2, :] = all_diagonal[place(order_s[s, me])].astype(F32)
    settle(got2.at[0, 0 : DEVICES - 1], in2.at[0], out2.at[0])
    for _ in begin(0, got2.at[0], aux_ref, root, block, x, y, z):
        pass
    done = pltpu.make_async_copy(root, out_any, local)
    done.start()
    for s in range(1, CAP):
        settle(got2.at[s, 0 : DEVICES - 1], in2.at[s], out2.at[s])
        g_ref[s - 1] = got2[s]
    done.wait()


def move(factors, target):
    vmem, dma = pltpu.VMEM, pltpu.SemaphoreType.DMA
    return pl.pallas_call(
        move_kernel,
        out_shape=(
            jax.ShapeDtypeStruct((CAP - 1, DEVICES, 8, 128), BF16),
            jax.ShapeDtypeStruct((16, 128), F32),
            jax.ShapeDtypeStruct((512, 512), F32),
        ),
        in_specs=[pl.BlockSpec(memory_space=pl.ANY), pl.BlockSpec(memory_space=vmem)],
        out_specs=[pl.BlockSpec(memory_space=vmem)] * 2 + [pl.BlockSpec(memory_space=pl.ANY)],
        scratch_shapes=[
            vmem((2, 512, 512), BF16),
            vmem((2, DEVICES, 8, 128), BF16),
            vmem((2, DEVICES, 8, 128), BF16),
            vmem((1, 128), F32),
            vmem((DEVICES, 1, 128), F32),
            vmem((2, 2, 128), BF16),
            vmem((2, DEVICES, 2, 128), BF16),
            vmem((CAP, DEVICES, 8, 128), BF16),
            vmem((CAP, DEVICES, 8, 128), BF16),
            vmem((8, 128), jnp.int32),
            pltpu.SMEM((8, 128), jnp.int32),
            vmem((512, 512), F32),
            vmem((512, 512), BF16),
            vmem((2, 512, 512), BF16),
            vmem((2, 512, 512), BF16),
            vmem((2, 512, 512), BF16),
            dma, dma, dma, dma, dma, dma, dma((CAP,)), dma((CAP,)), dma,
        ],
        compiler_params=pltpu.CompilerParams(collective_id=0, has_side_effects=True),
        name="move",
    )(factors, target)


def root_kernel(g_ref, aux_ref, first_any, out_any, root, block, x, y, z, sems):
    load = pltpu.make_async_copy(first_any, root.at[0], sems.at[0])
    load.start()
    works = [
        begin(s, g_ref.at[s - 1], aux_ref, root.at[s], *(r.at[s - 1] for r in (block, x, y, z)))
        for s in range(1, CAP)
    ]
    copies = [pltpu.make_async_copy(root.at[s], out_any.at[s], sems.at[s]) for s in range(CAP)]
    for step, _ in enumerate(itertools.zip_longest(*works)):
        if step == 3:
            load.wait()
            copies[0].start()
    for copy in copies[1:]:
        copy.start()
    for copy in copies:
        copy.wait()


def roots(moved, aux, first):
    vmem = pltpu.VMEM
    return pl.pallas_call(
        root_kernel,
        out_shape=jax.ShapeDtypeStruct((CAP, 512, 512), F32),
        in_specs=[
            pl.BlockSpec(memory_space=vmem),
            pl.BlockSpec(memory_space=vmem),
            pl.BlockSpec(memory_space=pl.ANY),
        ],
        out_specs=pl.BlockSpec(memory_space=pl.ANY),
        scratch_shapes=[
            vmem((CAP, 512, 512), F32),
            vmem((CAP - 1, 512, 512), BF16),
            vmem((CAP - 1, 2, 512, 512), BF16),
            vmem((CAP - 1, 2, 512, 512), BF16),
            vmem((CAP - 1, 2, 512, 512), BF16),
            pltpu.SemaphoreType.DMA((CAP,)),
        ],
        name="roots",
    )(moved, aux, first)


def shards(factors, target):
    return roots(*move(factors[0], target))[None]


def solution(mesh):
    finer = Mesh(mesh.devices.reshape(4, 2, 4, 4), AXES)
    placed = (P(AXES, None, None, None), P(AXES, None))
    return jax.shard_map(
        shards, mesh=finer, in_specs=placed, out_specs=P(AXES, None, None, None), check_vma=False
    )
```

```python
import itertools

import jax
import jax.numpy as jnp
from jax import lax
from jax.experimental import pallas as pl
from jax.experimental.pallas import tpu as pltpu
from jax.sharding import Mesh
from jax.sharding import PartitionSpec as P

AXES = ("y", "c", "z", "x")
MESH = pl.DeviceIdType.MESH
DEVICES = 128
HALF = 256
CAP = 3
GRANT = 32 << 20
F32 = jnp.float32
BF16 = jnp.bfloat16


def iota(shape, dim):
    return lax.broadcasted_iota(jnp.int32, shape, dim)


def total(value):
    return jnp.sum(jnp.sum(value, axis=1, keepdims=True), axis=0, keepdims=True)


def peer(k, here):
    y, c, z, x = here
    k = (k * 37) & (DEVICES - 1)
    there = (
        (y + ((k >> 4) & 3)) & 3,
        (c + (k >> 6)) & 1,
        (z + ((k >> 2) & 3)) & 3,
        (x + (k & 3)) & 3,
    )
    return there, ((there[0] * 2 + there[1]) * 4 + there[2]) * 4 + there[3]


def each_peer(here, do):
    for start, stop, unroll in ((1, 8, 7), (8, DEVICES, 8)):

        @pl.loop(start, stop, unroll=unroll)
        def _(k):
            do(*peer(k, here))


def pack(f_ref, t_ref, send1, facts_ref, diagonal_ref):
    row, col = iota((HALF, HALF), 0), iota((HALF, HALF), 1)
    sq = jnp.zeros((1, 1), F32)
    line = iota((2, 128), 0)
    for h in range(2):
        a = f_ref[h, 0:HALF, 0:HALF].astype(F32)
        b = f_ref[h, 0:HALF, HALF:]
        c = f_ref[h, HALF:, 0:HALF].astype(F32)
        d = f_ref[h, HALF:, HALF:].astype(F32)
        bf = b.astype(F32)
        sq = sq + total(a * a + bf * bf + c * c + d * d)
        v = jnp.where(row <= col, a, d).astype(BF16)
        diagonal = jnp.sum(jnp.where(row == col, d, 0.0), axis=0, keepdims=True)
        diagonal = jnp.where(line == 0, diagonal[:, 0:128], diagonal[:, 128:])
        diagonal_ref[h] = diagonal.astype(BF16)
        for part, w in enumerate((b, v)):
            for lanes in range(2):
                start = lanes * 64 + part * 32
                piece = w[:, lanes * 128 : lanes * 128 + 128]
                send1[h, start : start + 32] = piece.reshape(32, 8, 128)
    lane = iota((1, 128), 1)
    facts = jnp.where(lane == 0, t_ref[0:1, 0:1].astype(F32), 0.0)
    facts = jnp.where(lane == 1, t_ref[0:1, 1:2].astype(F32), facts)
    facts_ref[...] = jnp.where(lane == 2, sq, facts)


def plan(me, all_facts, order, aux_ref):
    facts = all_facts[:, 0, :]
    across = facts.T
    t0, t1 = facts[:, 0:1], facts[:, 1:2]
    r0, r1, sq = across[0:1, :], across[1:2, :], across[2:3, :]
    i, j = iota((DEVICES, DEVICES), 0), iota((DEVICES, DEVICES), 1)

    def same(a, b):
        return jnp.where(a == b, 1.0, 0.0)

    def along(value):
        return jnp.sum(value, axis=1, keepdims=True)

    before = j < i
    slot0 = along(jnp.where(before, same(r0, t0) + same(r1, t0), 0.0))
    slot1 = along(jnp.where(before, same(r0, t1) + same(r1, t1), 0.0)) + same(t0, t1)
    layer = along(jnp.where((i >> 4) == (j >> 4), sq, 0.0))
    fi, fj = i.astype(F32), j.astype(F32)
    line, lane = iota((8, 128), 0), iota((8, 128), 1)
    mine = iota((1, 128), 1) == me
    wanted = jnp.zeros((8, 128), F32)
    numbers = jnp.zeros((8, 128), F32)
    for s in range(CAP):
        first = jnp.where(t0 == fj, same(slot0, s), 0.0)
        second = jnp.where(t1 == fj, same(slot1, s), 0.0)
        both = first + second
        holds = jnp.sum(first * fi + second * (fi + DEVICES), axis=0, keepdims=True)
        filled = jnp.sum(both, axis=0, keepdims=True)
        layers = jnp.sum(both * layer, axis=0, keepdims=True)
        wanted = jnp.where(line == s, holds, wanted)
        my_filled = along(jnp.where(mine, filled, 0.0))
        my_layer = along(jnp.where(mine, layers, 0.0))
        scale = 2.0 * jnp.sqrt(jnp.where(my_filled > 0, my_layer, 16384.0) / 16384.0)
        inverse = jnp.where(my_filled > 0, 1.0 / scale, 0.0)
        factor = jnp.where(my_filled > 0, lax.rsqrt(jnp.sqrt(scale)), 0.0)
        numbers = jnp.where((line == s) & (lane == 0), inverse, numbers)
        numbers = jnp.where((line == s) & (lane == 1), factor, numbers)
    order[...] = wanted.astype(jnp.int32)
    aux_ref[8:16, :] = numbers


def dot(a, b):
    return jnp.dot(a, b, preferred_element_type=F32)


LEFT, RIGHT = slice(0, HALF), slice(HALF, 2 * HALF)


def tiles(ref):
    return [ref[r, c].astype(F32) for r, c in ((LEFT, LEFT), (LEFT, RIGHT), (RIGHT, RIGHT))]


def product(*pairs):
    right = sum(dot(a[...], b[:, RIGHT]) for a, b in pairs)
    corner = sum(dot(a[LEFT, :], b[:, LEFT]) for a, b in pairs)
    return [corner, right[LEFT], right[RIGHT]]


def times(a, b):
    return product((a[0], b[0]), (a[0], b[1]), (a[1], b[0]))


def keep(ref, value):
    places = (LEFT, LEFT), (LEFT, RIGHT), (RIGHT, RIGHT), (RIGHT, LEFT)
    for (r, c), tile in zip(places, (*value, value[1].T)):
        high = tile.astype(BF16)
        ref[0, r, c] = high
        ref[1, r, c] = (tile - high.astype(F32)).astype(BF16)


def unfold(g, diagonal, block):
    row, col = iota((HALF, HALF), 0), iota((HALF, HALF), 1)

    def whole(part):
        return jnp.concatenate(
            [
                g[lanes * 64 + part * 32 : lanes * 64 + part * 32 + 32].reshape(HALF, 128)
                for lanes in range(2)
            ],
            axis=1,
        )

    u = whole(0)
    v = whole(1).astype(F32)
    flipped = v.T
    block[LEFT, LEFT] = jnp.where(row <= col, v, flipped).astype(BF16)
    block[LEFT, RIGHT] = u
    block[RIGHT, LEFT] = u.astype(F32).T.astype(BF16)
    corner = jnp.where(row > col, v, jnp.where(row == col, diagonal, flipped))
    block[RIGHT, RIGHT] = corner.astype(BF16)


def newton(block, inverse, factor, out, x, y, z):
    eye = jnp.where(iota((HALF, HALF), 0) == iota((HALF, HALF), 1), 1.25, 0.0)
    eyes = (eye, 0.0, eye)
    q = inverse * 0.25
    square = product((block, block))
    keep(x, [1.25 * e - (2.5 * q) * a + (s * q) * q for e, a, s in zip(eyes, tiles(block), square)])
    yield
    keep(y, [t * q for t in product((x.at[0], block), (x.at[1], block))])
    yield
    step = [e - t for e, t in zip(eyes, times(x, y))]
    keep(z, step)
    yield
    square = times(z, z)
    keep(x, square)
    keep(y, [1.25 * t - s for t, s in zip(step, square)])
    yield
    keep(z, times(x, y))
    yield
    both = [1.25 * t - f for t, f in zip(step, times(x, z))]
    keep(y, both)
    yield
    rest = product((y.at[0], block), (y.at[1], block))
    root = [(1.25 * t - r * q) * factor for t, r in zip(both, rest)]
    out[LEFT, LEFT] = root[0]
    out[LEFT, RIGHT] = root[1]
    out[RIGHT, RIGHT] = root[2]
    out[RIGHT, LEFT] = root[1].T


def begin(s, g, aux_ref, out, block, x, y, z):
    unfold(g, jnp.concatenate([aux_ref[2 * s : 2 * s + 1], aux_ref[2 * s + 1 : 2 * s + 2]], axis=1), block)
    return newton(block, aux_ref[8 + s : 9 + s, 0:1], aux_ref[8 + s : 9 + s, 1:2], out, x, y, z)


def move_kernel(
    f_hbm, t_hbm, g_any, aux_ref, out_any,
    t_ref, f_ref, send1, got1, facts, all_facts, diagonal, all_diagonal, send2, got2, order, order_s,
    root, block, x, y, z,
    facts_out, facts_in, diagonal_out, diagonal_in, out1, in1, out2, in2, local, stored,
):
    here = tuple(lax.axis_index(a) for a in AXES)
    me = ((here[0] * 2 + here[1]) * 4 + here[2]) * 4 + here[3]
    loads = [
        pltpu.make_async_copy(f_hbm, f_ref, stored.at[0]),
        pltpu.make_async_copy(t_hbm, t_ref, stored.at[1]),
    ]
    for load in loads:
        load.start()
    barrier = pltpu.get_barrier_semaphore()
    each_peer(
        here,
        lambda there, _: pl.semaphore_signal(barrier, 1, device_id=there, device_id_type=MESH),
    )
    for load in loads:
        load.wait()
    pack(f_ref, t_ref, send1, facts, diagonal)
    pl.semaphore_wait(barrier, DEVICES - 1)

    def send(source, target, gone, came):
        def start(there, index):
            pltpu.make_async_remote_copy(
                src_ref=source(index), dst_ref=target, send_sem=gone, recv_sem=came,
                device_id=there, device_id_type=MESH,
            ).start()

        each_peer(here, start)

    def settle(buffer, *sems):
        for sem in sems:
            pltpu.make_async_copy(buffer, buffer, sem).wait()

    send(lambda index: facts, all_facts.at[me], facts_out, facts_in)
    send(lambda index: send1.at[:, index], got1.at[:, me], out1, in1)
    send(lambda index: diagonal, all_diagonal.at[:, me], diagonal_out, diagonal_in)
    all_facts[me] = facts[...]
    got1[:, me] = send1[:, me]
    all_diagonal[:, me] = diagonal[...]
    settle(all_facts.at[0 : DEVICES - 1], facts_in, facts_out)
    plan(me, all_facts, order, aux_ref)
    copy = pltpu.make_async_copy(order, order_s, local)
    copy.start()
    copy.wait()
    settle(got1.at[:, 0 : DEVICES - 1], in1, out1)

    def place(block):
        return (block >> 7) & 1, block & (DEVICES - 1)

    for s in range(CAP):

        @pl.loop(0, DEVICES, unroll=8)
        def _(d, s=s):
            send2[s, d] = got1[place(order_s[s, d])]

        send(lambda index, s=s: send2.at[s, index], got2.at[s, me], out2.at[s], in2.at[s])
        got2[s, me] = send2[s, me]
    settle(all_diagonal.at[:, 0 : DEVICES - 1], diagonal_in, diagonal_out)
    for s in range(CAP):
        aux_ref[2 * s : 2 * s + 2, :] = all_diagonal[place(order_s[s, me])].astype(F32)
    settle(got2.at[0, 0 : DEVICES - 1], in2.at[0], out2.at[0])
    stores = [pltpu.make_async_copy(root, out_any, stored.at[0])]
    stores += [pltpu.make_async_copy(got2.at[s], g_any.at[s - 1], stored.at[s]) for s in range(1, CAP)]

    def store(s):
        settle(got2.at[s, 0 : DEVICES - 1], in2.at[s], out2.at[s])
        stores[s].start()

    for step, _ in enumerate(begin(0, got2.at[0], aux_ref, root, block, x, y, z)):
        if step == 4:
            store(1)
    stores[0].start()
    store(2)
    for copy in stores:
        copy.wait()


def move(factors, target):
    vmem, dma = pltpu.VMEM, pltpu.SemaphoreType.DMA
    return pl.pallas_call(
        move_kernel,
        out_shape=(
            jax.ShapeDtypeStruct((CAP - 1, DEVICES, 8, 128), BF16),
            jax.ShapeDtypeStruct((16, 128), F32),
            jax.ShapeDtypeStruct((512, 512), F32),
        ),
        in_specs=[pl.BlockSpec(memory_space=pltpu.HBM)] * 2,
        out_specs=[pl.BlockSpec(memory_space=m) for m in (pl.ANY, vmem, pl.ANY)],
        scratch_shapes=[
            vmem((1, 2), jnp.int32),
            vmem((2, 512, 512), BF16),
            vmem((2, DEVICES, 8, 128), BF16),
            vmem((2, DEVICES, 8, 128), BF16),
            vmem((1, 128), F32),
            vmem((DEVICES, 1, 128), F32),
            vmem((2, 2, 128), BF16),
            vmem((2, DEVICES, 2, 128), BF16),
            vmem((CAP, DEVICES, 8, 128), BF16),
            vmem((CAP, DEVICES, 8, 128), BF16),
            vmem((8, 128), jnp.int32),
            pltpu.SMEM((8, 128), jnp.int32),
            vmem((512, 512), F32),
            vmem((512, 512), BF16),
            vmem((2, 512, 512), BF16),
            vmem((2, 512, 512), BF16),
            vmem((2, 512, 512), BF16),
            dma, dma, dma, dma, dma, dma, dma((CAP,)), dma((CAP,)), dma, dma((CAP,)),
        ],
        compiler_params=pltpu.CompilerParams(collective_id=0, has_side_effects=True, vmem_limit_bytes=GRANT),
        name="move",
    )(factors, target)


def root_kernel(g_ref, aux_ref, first_ref, out_any, root, block, x, y, z, sems):
    copies = [pltpu.make_async_copy(first_ref, out_any.at[0], sems.at[0])]
    copies[0].start()
    works = []
    for s in range(1, CAP):
        places = (r.at[s - 1] for r in (root, block, x, y, z))
        works.append(begin(s, g_ref.at[s - 1], aux_ref, *places))
        copies.append(pltpu.make_async_copy(root.at[s - 1], out_any.at[s], sems.at[s]))
    for step in range(7):
        for s, work in enumerate(works):
            next(work, None)
            if step == 6:
                copies[s + 1].start()
    for copy in copies:
        copy.wait()


def roots(moved, aux, first):
    vmem = pltpu.VMEM
    return pl.pallas_call(
        root_kernel,
        out_shape=jax.ShapeDtypeStruct((CAP, 512, 512), F32),
        in_specs=[pl.BlockSpec(memory_space=vmem)] * 3,
        out_specs=pl.BlockSpec(memory_space=pl.ANY),
        scratch_shapes=[
            vmem((CAP - 1, 512, 512), F32),
            vmem((CAP - 1, 512, 512), BF16),
            vmem((CAP - 1, 2, 512, 512), BF16),
            vmem((CAP - 1, 2, 512, 512), BF16),
            vmem((CAP - 1, 2, 512, 512), BF16),
            pltpu.SemaphoreType.DMA((CAP,)),
        ],
        compiler_params=pltpu.CompilerParams(vmem_limit_bytes=GRANT),
        name="roots",
    )(moved, aux, first)


def shards(factors, target):
    return roots(*move(pltpu.with_memory_space_constraint(factors[0], pltpu.HBM), pltpu.with_memory_space_constraint(target.T, pltpu.HBM)))[None]


def solution(mesh):
    finer = Mesh(mesh.devices.reshape(4, 2, 4, 4), AXES)
    placed = (P(AXES, None, None, None), P(AXES, None))
    return jax.shard_map(
        shards, mesh=finer, in_specs=placed, out_specs=P(AXES, None, None, None), check_vma=False
    )
```

```python
import itertools

import jax
import jax.numpy as jnp
from jax import lax
from jax.experimental import pallas as pl
from jax.experimental.pallas import tpu as pltpu
from jax.sharding import Mesh
from jax.sharding import PartitionSpec as P

AXES = ("y", "c", "z", "x")
MESH = pl.DeviceIdType.MESH
DEVICES = 128
HALF = 256
CAP = 3
GRANT = 32 << 20
F32 = jnp.float32
BF16 = jnp.bfloat16


def iota(shape, dim):
    return lax.broadcasted_iota(jnp.int32, shape, dim)


def total(value):
    return jnp.sum(jnp.sum(value, axis=1, keepdims=True), axis=0, keepdims=True)


def step_of(digit):
    return (0x36 >> (2 * (digit & 3))) & 3


def peer(k, here):
    y, c, z, x = here
    there = (
        (y + step_of(k >> 4)) & 3,
        (c + 1 - (k >> 6)) & 1,
        (z + step_of(k >> 2)) & 3,
        (x + step_of(k)) & 3,
    )
    return there, ((there[0] * 2 + there[1]) * 4 + there[2]) * 4 + there[3]


def each_peer(here, do):
    @pl.loop(0, DEVICES - 1, unroll=DEVICES - 1)
    def _(k):
        do(*peer(k, here))


def pack(f_ref, t_ref, send1, facts_ref, diagonal_ref):
    row, col = iota((HALF, HALF), 0), iota((HALF, HALF), 1)
    sq = jnp.zeros((1, 1), F32)
    line = iota((2, 128), 0)
    for h in range(2):
        a = f_ref[h, 0:HALF, 0:HALF].astype(F32)
        b = f_ref[h, 0:HALF, HALF:]
        d = f_ref[h, HALF:, HALF:].astype(F32)
        bf = b.astype(F32)
        sq = sq + total(a * a + 2.0 * (bf * bf) + d * d)
        v = jnp.where(row <= col, a, d).astype(BF16)
        diagonal = jnp.sum(jnp.where(row == col, d, 0.0), axis=0, keepdims=True)
        diagonal = jnp.where(line == 0, diagonal[:, 0:128], diagonal[:, 128:])
        diagonal_ref[h] = diagonal.astype(BF16)
        for part, w in enumerate((b, v)):
            for lanes in range(2):
                start = lanes * 64 + part * 32
                piece = w[:, lanes * 128 : lanes * 128 + 128]
                send1[h, start : start + 32] = piece.reshape(32, 8, 128)
    lane = iota((1, 128), 1)
    facts = jnp.where(lane == 0, t_ref[0:1, 0:1].astype(F32), 0.0)
    facts = jnp.where(lane == 1, t_ref[0:1, 1:2].astype(F32), facts)
    facts_ref[...] = jnp.where(lane == 2, sq, facts)


def plan(me, all_facts, order, aux_ref):
    facts = all_facts[:, 0, :]
    across = facts.T
    t0, t1 = facts[:, 0:1], facts[:, 1:2]
    r0, r1, sq = across[0:1, :], across[1:2, :], across[2:3, :]
    i, j = iota((DEVICES, DEVICES), 0), iota((DEVICES, DEVICES), 1)

    def same(a, b):
        return jnp.where(a == b, 1.0, 0.0)

    def along(value):
        return jnp.sum(value, axis=1, keepdims=True)

    before = j < i
    slot0 = along(jnp.where(before, same(r0, t0) + same(r1, t0), 0.0))
    slot1 = along(jnp.where(before, same(r0, t1) + same(r1, t1), 0.0)) + same(t0, t1)
    layer = along(jnp.where((i >> 4) == (j >> 4), sq, 0.0))
    fi, fj = i.astype(F32), j.astype(F32)
    line, lane = iota((8, 128), 0), iota((8, 128), 1)
    mine = iota((1, 128), 1) == me
    wanted = jnp.zeros((8, 128), F32)
    numbers = jnp.zeros((8, 128), F32)
    for s in range(CAP):
        first = jnp.where(t0 == fj, same(slot0, s), 0.0)
        second = jnp.where(t1 == fj, same(slot1, s), 0.0)
        both = first + second
        holds = jnp.sum(first * fi + second * (fi + DEVICES), axis=0, keepdims=True)
        filled = jnp.sum(both, axis=0, keepdims=True)
        layers = jnp.sum(both * layer, axis=0, keepdims=True)
        wanted = jnp.where(line == s, holds, wanted)
        my_filled = along(jnp.where(mine, filled, 0.0))
        my_layer = along(jnp.where(mine, layers, 0.0))
        scale = 2.0 * jnp.sqrt(jnp.where(my_filled > 0, my_layer, 16384.0) / 16384.0)
        inverse = jnp.where(my_filled > 0, 1.0 / scale, 0.0)
        factor = jnp.where(my_filled > 0, lax.rsqrt(jnp.sqrt(scale)), 0.0)
        numbers = jnp.where((line == s) & (lane == 0), inverse, numbers)
        numbers = jnp.where((line == s) & (lane == 1), factor, numbers)
    order[...] = wanted.astype(jnp.int32)
    aux_ref[8:16, :] = numbers


def dot(a, b):
    return jnp.dot(a, b, preferred_element_type=F32)


LEFT, RIGHT = slice(0, HALF), slice(HALF, 2 * HALF)


def tiles(ref):
    return [ref[r, c].astype(F32) for r, c in ((LEFT, LEFT), (LEFT, RIGHT), (RIGHT, RIGHT))]


def product(*pairs):
    right = sum(dot(a[...], b[:, RIGHT]) for a, b in pairs)
    corner = sum(dot(a[LEFT, :], b[:, LEFT]) for a, b in pairs)
    return [corner, right[LEFT], right[RIGHT]]


def times(a, b):
    return product((a[0], b[0]), (a[0], b[1]), (a[1], b[0]))


def squared(a):
    high = product((a.at[0], a.at[0]))
    cross = dot(a[0], a[1])
    sides = ((LEFT, LEFT), (LEFT, RIGHT), (RIGHT, RIGHT))
    return [t + (cross[r, c] + cross[c, r].T) for t, (r, c) in zip(high, sides)]


def keep(ref, value):
    places = (LEFT, LEFT), (LEFT, RIGHT), (RIGHT, RIGHT), (RIGHT, LEFT)
    for (r, c), tile in zip(places, (*value, value[1].T)):
        high = tile.astype(BF16)
        ref[0, r, c] = high
        ref[1, r, c] = (tile - high.astype(F32)).astype(BF16)


def unfold(g, diagonal, block):
    row, col = iota((HALF, HALF), 0), iota((HALF, HALF), 1)

    def whole(part):
        return jnp.concatenate(
            [
                g[lanes * 64 + part * 32 : lanes * 64 + part * 32 + 32].reshape(HALF, 128)
                for lanes in range(2)
            ],
            axis=1,
        )

    u = whole(0)
    v = whole(1).astype(F32)
    flipped = v.T
    block[LEFT, LEFT] = jnp.where(row <= col, v, flipped).astype(BF16)
    block[LEFT, RIGHT] = u
    block[RIGHT, LEFT] = u.astype(F32).T.astype(BF16)
    corner = jnp.where(row > col, v, jnp.where(row == col, diagonal, flipped))
    block[RIGHT, RIGHT] = corner.astype(BF16)


def newton(block, inverse, factor, out, x, y, z):
    eye = jnp.where(iota((HALF, HALF), 0) == iota((HALF, HALF), 1), 1.25, 0.0)
    eyes = (eye, 0.0, eye)
    q = inverse * 0.25
    square = product((block, block))
    keep(x, [1.25 * e - (2.5 * q) * a + (s * q) * q for e, a, s in zip(eyes, tiles(block), square)])
    yield
    keep(y, squared(x))
    yield
    step = [e - t * q for e, t in zip(eyes, product((y.at[0], block), (y.at[1], block)))]
    keep(z, step)
    yield
    square = squared(z)
    keep(x, square)
    keep(y, [1.25 * t - s for t, s in zip(step, square)])
    yield
    keep(z, squared(x))
    yield
    both = [1.25 * t - f for t, f in zip(step, times(z, y))]
    keep(x, both)
    yield
    rest = product((x.at[0], block), (x.at[1], block))
    root = [(1.25 * t - r * q) * factor for t, r in zip(both, rest)]
    out[LEFT, LEFT] = root[0]
    out[LEFT, RIGHT] = root[1]
    out[RIGHT, RIGHT] = root[2]
    out[RIGHT, LEFT] = root[1].T


def begin(s, g, aux_ref, out, block, x, y, z):
    unfold(g, jnp.concatenate([aux_ref[2 * s : 2 * s + 1], aux_ref[2 * s + 1 : 2 * s + 2]], axis=1), block)
    return newton(block, aux_ref[8 + s : 9 + s, 0:1], aux_ref[8 + s : 9 + s, 1:2], out, x, y, z)


def move_kernel(
    f_hbm, t_hbm, g_any, aux_ref, out_any,
    t_ref, f_ref, send1, got1, facts, all_facts, diagonal, all_diagonal, send2, got2, order, order_s,
    root, block, x, y, z,
    facts_out, facts_in, diagonal_out, diagonal_in, out1, in1, out2, in2, local, stored,
):
    here = tuple(lax.axis_index(a) for a in AXES)
    me = ((here[0] * 2 + here[1]) * 4 + here[2]) * 4 + here[3]
    loads = [
        pltpu.make_async_copy(f_hbm, f_ref, stored.at[0]),
        pltpu.make_async_copy(t_hbm, t_ref, stored.at[1]),
    ]
    for load in loads:
        load.start()
    barrier = pltpu.get_barrier_semaphore()
    each_peer(
        here,
        lambda there, _: pl.semaphore_signal(barrier, 1, device_id=there, device_id_type=MESH),
    )
    for load in loads:
        load.wait()
    pack(f_ref, t_ref, send1, facts, diagonal)
    pl.semaphore_wait(barrier, DEVICES - 1)

    def send(source, target, gone, came):
        def start(there, index):
            pltpu.make_async_remote_copy(
                src_ref=source(index), dst_ref=target, send_sem=gone, recv_sem=came,
                device_id=there, device_id_type=MESH,
            ).start()

        each_peer(here, start)

    def settle(buffer, *sems):
        for sem in sems:
            pltpu.make_async_copy(buffer, buffer, sem).wait()

    send(lambda index: facts, all_facts.at[me], facts_out, facts_in)
    send(lambda index: send1.at[:, index], got1.at[:, me], out1, in1)
    send(lambda index: diagonal, all_diagonal.at[:, me], diagonal_out, diagonal_in)
    all_facts[me] = facts[...]
    got1[:, me] = send1[:, me]
    all_diagonal[:, me] = diagonal[...]
    settle(all_facts.at[0 : DEVICES - 1], facts_in, facts_out)
    plan(me, all_facts, order, aux_ref)
    copy = pltpu.make_async_copy(order, order_s, local)
    copy.start()
    copy.wait()
    settle(got1.at[:, 0 : DEVICES - 1], in1, out1)

    def place(block):
        return (block >> 7) & 1, block & (DEVICES - 1)

    for s in range(CAP):

        @pl.loop(0, DEVICES, unroll=8)
        def _(d, s=s):
            send2[s, d] = got1[place(order_s[s, d])]

        send(lambda index, s=s: send2.at[s, index], got2.at[s, me], out2.at[s], in2.at[s])
        got2[s, me] = send2[s, me]
    settle(all_diagonal.at[:, 0 : DEVICES - 1], diagonal_in, diagonal_out)
    for s in range(CAP):
        aux_ref[2 * s : 2 * s + 2, :] = all_diagonal[place(order_s[s, me])].astype(F32)
    settle(got2.at[0, 0 : DEVICES - 1], in2.at[0], out2.at[0])
    stores = [pltpu.make_async_copy(root, out_any, stored.at[0])]
    stores += [pltpu.make_async_copy(got2.at[s], g_any.at[s - 1], stored.at[s]) for s in range(1, CAP)]

    def store(s):
        settle(got2.at[s, 0 : DEVICES - 1], in2.at[s], out2.at[s])
        stores[s].start()

    for step, _ in enumerate(begin(0, got2.at[0], aux_ref, root, block, x, y, z)):
        if step == 4:
            store(1)
    stores[0].start()
    store(2)
    for copy in stores:
        copy.wait()


def move(factors, target):
    vmem, dma = pltpu.VMEM, pltpu.SemaphoreType.DMA
    return pl.pallas_call(
        move_kernel,
        out_shape=(
            jax.ShapeDtypeStruct((CAP - 1, DEVICES, 8, 128), BF16),
            jax.ShapeDtypeStruct((16, 128), F32),
            jax.ShapeDtypeStruct((512, 512), F32),
        ),
        in_specs=[pl.BlockSpec(memory_space=pltpu.HBM)] * 2,
        out_specs=[pl.BlockSpec(memory_space=m) for m in (pl.ANY, vmem, pl.ANY)],
        scratch_shapes=[
            vmem((1, 2), jnp.int32),
            vmem((2, 512, 512), BF16),
            vmem((2, DEVICES, 8, 128), BF16),
            vmem((2, DEVICES, 8, 128), BF16),
            vmem((1, 128), F32),
            vmem((DEVICES, 1, 128), F32),
            vmem((2, 2, 128), BF16),
            vmem((2, DEVICES, 2, 128), BF16),
            vmem((CAP, DEVICES, 8, 128), BF16),
            vmem((CAP, DEVICES, 8, 128), BF16),
            vmem((8, 128), jnp.int32),
            pltpu.SMEM((8, 128), jnp.int32),
            vmem((512, 512), F32),
            vmem((512, 512), BF16),
            vmem((2, 512, 512), BF16),
            vmem((2, 512, 512), BF16),
            vmem((2, 512, 512), BF16),
            dma, dma, dma, dma, dma, dma, dma((CAP,)), dma((CAP,)), dma, dma((CAP,)),
        ],
        compiler_params=pltpu.CompilerParams(collective_id=0, has_side_effects=True, vmem_limit_bytes=GRANT),
        name="move",
    )(factors, target)


def root_kernel(g_ref, aux_ref, first_ref, out_any, root, block, x, y, z, sems):
    copies = [pltpu.make_async_copy(first_ref, out_any.at[0], sems.at[0])]
    copies[0].start()
    works = []
    for s in range(1, CAP):
        places = (r.at[s - 1] for r in (root, block, x, y, z))
        works.append(begin(s, g_ref.at[s - 1], aux_ref, *places))
        copies.append(pltpu.make_async_copy(root.at[s - 1], out_any.at[s], sems.at[s]))
    for step in range(7):
        for s, work in enumerate(works):
            next(work, None)
            if step == 6:
                copies[s + 1].start()
    for copy in copies:
        copy.wait()


def roots(moved, aux, first):
    vmem = pltpu.VMEM
    return pl.pallas_call(
        root_kernel,
        out_shape=jax.ShapeDtypeStruct((CAP, 512, 512), F32),
        in_specs=[pl.BlockSpec(memory_space=vmem)] * 3,
        out_specs=pl.BlockSpec(memory_space=pl.ANY),
        scratch_shapes=[
            vmem((CAP - 1, 512, 512), F32),
            vmem((CAP - 1, 512, 512), BF16),
            vmem((CAP - 1, 2, 512, 512), BF16),
            vmem((CAP - 1, 2, 512, 512), BF16),
            vmem((CAP - 1, 2, 512, 512), BF16),
            pltpu.SemaphoreType.DMA((CAP,)),
        ],
        compiler_params=pltpu.CompilerParams(vmem_limit_bytes=GRANT),
        name="roots",
    )(moved, aux, first)


def shards(factors, target):
    return roots(*move(pltpu.with_memory_space_constraint(factors[0], pltpu.HBM), pltpu.with_memory_space_constraint(target.T, pltpu.HBM)))[None]


def solution(mesh):
    finer = Mesh(mesh.devices.reshape(4, 2, 4, 4), AXES)
    placed = (P(AXES, None, None, None), P(AXES, None))
    return jax.shard_map(
        shards, mesh=finer, in_specs=placed, out_specs=P(AXES, None, None, None), check_vma=False
    )
```

```python
import itertools

import jax
import jax.numpy as jnp
from jax import lax
from jax.experimental import pallas as pl
from jax.experimental.pallas import tpu as pltpu
from jax.sharding import Mesh
from jax.sharding import PartitionSpec as P

AXES = ("y", "c", "z", "x")
MESH = pl.DeviceIdType.MESH
DEVICES = 128
HALF = 256
CAP = 3
GRANT = 32 << 20
F32 = jnp.float32
BF16 = jnp.bfloat16


def iota(shape, dim):
    return lax.broadcasted_iota(jnp.int32, shape, dim)


def total(value):
    return jnp.sum(jnp.sum(value, axis=1, keepdims=True), axis=0, keepdims=True)


def step_of(digit):
    return (0x36 >> (2 * (digit & 3))) & 3


def peer(k, here):
    y, c, z, x = here
    there = (
        (y + step_of(k >> 4)) & 3,
        (c + 1 - (k >> 6)) & 1,
        (z + step_of(k >> 2)) & 3,
        (x + step_of(k)) & 3,
    )
    return there, ((there[0] * 2 + there[1]) * 4 + there[2]) * 4 + there[3]


def each_peer(here, do):
    @pl.loop(0, DEVICES - 1, unroll=DEVICES - 1)
    def _(k):
        do(*peer(k, here))


def pack(f_ref, t_ref, send1, facts_ref, diagonal_ref):
    row, col = iota((HALF, HALF), 0), iota((HALF, HALF), 1)
    sq = jnp.zeros((1, 1), F32)
    line = iota((2, 128), 0)
    for h in range(2):
        a = f_ref[h, 0:HALF, 0:HALF].astype(F32)
        b = f_ref[h, 0:HALF, HALF:]
        d = f_ref[h, HALF:, HALF:].astype(F32)
        bf = b.astype(F32)
        sq = sq + total(a * a + 2.0 * (bf * bf) + d * d)
        v = jnp.where(row <= col, a, d).astype(BF16)
        diagonal = jnp.sum(jnp.where(row == col, d, 0.0), axis=0, keepdims=True)
        diagonal = jnp.where(line == 0, diagonal[:, 0:128], diagonal[:, 128:])
        diagonal_ref[h] = diagonal.astype(BF16)
        for part, w in enumerate((b, v)):
            for lanes in range(2):
                start = lanes * 64 + part * 32
                piece = w[:, lanes * 128 : lanes * 128 + 128]
                send1[h, start : start + 32] = piece.reshape(32, 8, 128)
    lane = iota((1, 128), 1)
    facts = jnp.where(lane == 0, t_ref[0:1, 0:1].astype(F32), 0.0)
    facts = jnp.where(lane == 1, t_ref[0:1, 1:2].astype(F32), facts)
    facts_ref[...] = jnp.where(lane == 2, sq, facts)


def plan(me, all_facts, order, aux_ref):
    facts = all_facts[:, 0, :]
    across = facts.T
    t0, t1 = facts[:, 0:1], facts[:, 1:2]
    r0, r1, sq = across[0:1, :], across[1:2, :], across[2:3, :]
    i, j = iota((DEVICES, DEVICES), 0), iota((DEVICES, DEVICES), 1)

    def same(a, b):
        return jnp.where(a == b, 1.0, 0.0)

    def along(value):
        return jnp.sum(value, axis=1, keepdims=True)

    before = j < i
    slot0 = along(jnp.where(before, same(r0, t0) + same(r1, t0), 0.0))
    slot1 = along(jnp.where(before, same(r0, t1) + same(r1, t1), 0.0)) + same(t0, t1)
    layer = along(jnp.where((i >> 4) == (j >> 4), sq, 0.0))
    fi, fj = i.astype(F32), j.astype(F32)
    line, lane = iota((8, 128), 0), iota((8, 128), 1)
    mine = iota((1, 128), 1) == me
    wanted = jnp.zeros((8, 128), F32)
    numbers = jnp.zeros((8, 128), F32)
    for s in range(CAP):
        first = jnp.where(t0 == fj, same(slot0, s), 0.0)
        second = jnp.where(t1 == fj, same(slot1, s), 0.0)
        both = first + second
        holds = jnp.sum(first * fi + second * (fi + DEVICES), axis=0, keepdims=True)
        filled = jnp.sum(both, axis=0, keepdims=True)
        layers = jnp.sum(both * layer, axis=0, keepdims=True)
        wanted = jnp.where(line == s, holds, wanted)
        my_filled = along(jnp.where(mine, filled, 0.0))
        my_layer = along(jnp.where(mine, layers, 0.0))
        scale = 2.0 * jnp.sqrt(jnp.where(my_filled > 0, my_layer, 16384.0) / 16384.0)
        inverse = jnp.where(my_filled > 0, 1.0 / scale, 0.0)
        factor = jnp.where(my_filled > 0, lax.rsqrt(jnp.sqrt(scale)), 0.0)
        numbers = jnp.where((line == s) & (lane == 0), inverse, numbers)
        numbers = jnp.where((line == s) & (lane == 1), factor, numbers)
    order[...] = wanted.astype(jnp.int32)
    aux_ref[8:16, :] = numbers


def dot(a, b):
    return jnp.dot(a, b, preferred_element_type=F32)


LEFT, RIGHT = slice(0, HALF), slice(HALF, 2 * HALF)


def tiles(ref):
    return [ref[r, c].astype(F32) for r, c in ((LEFT, LEFT), (LEFT, RIGHT), (RIGHT, RIGHT))]


def product(*pairs):
    right = sum(dot(a[...], b[:, RIGHT]) for a, b in pairs)
    corner = sum(dot(a[LEFT, :], b[:, LEFT]) for a, b in pairs)
    return [corner, right[LEFT], right[RIGHT]]


def times(a, b):
    return product((a[0], b[0]), (a[0], b[1]), (a[1], b[0]))


def squared(a):
    high = product((a.at[0], a.at[0]))
    cross = dot(a[0], a[1])
    sides = ((LEFT, LEFT), (LEFT, RIGHT), (RIGHT, RIGHT))
    return [t + (cross[r, c] + cross[c, r].T) for t, (r, c) in zip(high, sides)]


def keep(ref, value):
    places = (LEFT, LEFT), (LEFT, RIGHT), (RIGHT, RIGHT), (RIGHT, LEFT)
    for (r, c), tile in zip(places, (*value, value[1].T)):
        high = tile.astype(BF16)
        ref[0, r, c] = high
        ref[1, r, c] = (tile - high.astype(F32)).astype(BF16)


def unfold(g, diagonal, block):
    row, col = iota((HALF, HALF), 0), iota((HALF, HALF), 1)

    def whole(part):
        return jnp.concatenate(
            [
                g[lanes * 64 + part * 32 : lanes * 64 + part * 32 + 32].reshape(HALF, 128)
                for lanes in range(2)
            ],
            axis=1,
        )

    u = whole(0)
    v = whole(1).astype(F32)
    flipped = v.T
    block[LEFT, LEFT] = jnp.where(row <= col, v, flipped).astype(BF16)
    block[LEFT, RIGHT] = u
    block[RIGHT, LEFT] = u.astype(F32).T.astype(BF16)
    corner = jnp.where(row > col, v, jnp.where(row == col, diagonal, flipped))
    block[RIGHT, RIGHT] = corner.astype(BF16)


def newton(block, inverse, factor, out, x, y, z):
    eye = jnp.where(iota((HALF, HALF), 0) == iota((HALF, HALF), 1), 1.25, 0.0)
    eyes = (eye, 0.0, eye)
    q = inverse * 0.25
    square = product((block, block))
    keep(x, [1.25 * e - (2.5 * q) * a + (s * q) * q for e, a, s in zip(eyes, tiles(block), square)])
    yield
    keep(y, squared(x))
    yield
    step = [e - t * q for e, t in zip(eyes, product((y.at[0], block), (y.at[1], block)))]
    keep(z, step)
    yield
    square = squared(z)
    keep(x, square)
    keep(y, [1.25 * t - s for t, s in zip(step, square)])
    yield
    keep(z, squared(x))
    yield
    both = [1.25 * t - f for t, f in zip(step, times(z, y))]
    keep(x, both)
    yield
    rest = product((x.at[0], block), (x.at[1], block))
    root = [(1.25 * t - r * q) * factor for t, r in zip(both, rest)]
    out[LEFT, LEFT] = root[0]
    out[LEFT, RIGHT] = root[1]
    out[RIGHT, RIGHT] = root[2]
    out[RIGHT, LEFT] = root[1].T


def begin(s, g, aux_ref, out, block, x, y, z):
    unfold(g, jnp.concatenate([aux_ref[2 * s : 2 * s + 1], aux_ref[2 * s + 1 : 2 * s + 2]], axis=1), block)
    return newton(block, aux_ref[8 + s : 9 + s, 0:1], aux_ref[8 + s : 9 + s, 1:2], out, x, y, z)


def move_kernel(
    f_hbm, t_hbm, g_ref, aux_ref, first_ref,
    t_ref, f_ref, send1, got1, facts, all_facts, diagonal, all_diagonal, send2, got2, order, order_s,
    block, x, y, z,
    facts_out, facts_in, diagonal_out, diagonal_in, out1, in1, out2, in2, local, loaded,
):
    here = tuple(lax.axis_index(a) for a in AXES)
    me = ((here[0] * 2 + here[1]) * 4 + here[2]) * 4 + here[3]
    loads = [
        pltpu.make_async_copy(f_hbm, f_ref, loaded.at[0]),
        pltpu.make_async_copy(t_hbm, t_ref, loaded.at[1]),
    ]
    for load in loads:
        load.start()
    barrier = pltpu.get_barrier_semaphore()
    each_peer(
        here,
        lambda there, _: pl.semaphore_signal(barrier, 1, device_id=there, device_id_type=MESH),
    )
    for load in loads:
        load.wait()
    pack(f_ref, t_ref, send1, facts, diagonal)
    pl.semaphore_wait(barrier, DEVICES - 1)

    def send(source, target, gone, came):
        def start(there, index):
            pltpu.make_async_remote_copy(
                src_ref=source(index), dst_ref=target, send_sem=gone, recv_sem=came,
                device_id=there, device_id_type=MESH,
            ).start()

        each_peer(here, start)

    def settle(buffer, *sems):
        for sem in sems:
            pltpu.make_async_copy(buffer, buffer, sem).wait()

    send(lambda index: facts, all_facts.at[me], facts_out, facts_in)
    send(lambda index: send1.at[:, index], got1.at[:, me], out1, in1)
    send(lambda index: diagonal, all_diagonal.at[:, me], diagonal_out, diagonal_in)
    all_facts[me] = facts[...]
    got1[:, me] = send1[:, me]
    all_diagonal[:, me] = diagonal[...]
    settle(all_facts.at[0 : DEVICES - 1], facts_in, facts_out)
    plan(me, all_facts, order, aux_ref)
    copy = pltpu.make_async_copy(order, order_s, local)
    copy.start()
    copy.wait()
    settle(got1.at[:, 0 : DEVICES - 1], in1, out1)

    def place(block):
        return (block >> 7) & 1, block & (DEVICES - 1)

    for s in range(CAP):

        @pl.loop(0, DEVICES, unroll=32)
        def _(d, s=s):
            send2[s, d] = got1[place(order_s[s, d])]

        send(lambda index, s=s: send2.at[s, index], got2.at[s, me], out2.at[s], in2.at[s])
        got2[s, me] = send2[s, me]
    settle(all_diagonal.at[:, 0 : DEVICES - 1], diagonal_in, diagonal_out)
    for s in range(CAP):
        aux_ref[2 * s : 2 * s + 2, :] = all_diagonal[place(order_s[s, me])].astype(F32)
    settle(got2.at[0, 0 : DEVICES - 1], in2.at[0], out2.at[0])

    def store(s):
        settle(got2.at[s, 0 : DEVICES - 1], in2.at[s], out2.at[s])
        g_ref[s - 1] = got2[s]

    for step, _ in enumerate(begin(0, got2.at[0], aux_ref, first_ref, block, x, y, z)):
        if step == 5:
            store(1)
    store(2)


def move(factors, target):
    vmem, dma = pltpu.VMEM, pltpu.SemaphoreType.DMA
    return pl.pallas_call(
        move_kernel,
        out_shape=(
            jax.ShapeDtypeStruct((CAP - 1, DEVICES, 8, 128), BF16),
            jax.ShapeDtypeStruct((16, 128), F32),
            jax.ShapeDtypeStruct((512, 512), F32),
        ),
        in_specs=[pl.BlockSpec(memory_space=pltpu.HBM)] * 2,
        out_specs=[pl.BlockSpec(memory_space=vmem)] * 3,
        scratch_shapes=[
            vmem((1, 2), jnp.int32),
            vmem((2, 512, 512), BF16),
            vmem((2, DEVICES, 8, 128), BF16),
            vmem((2, DEVICES, 8, 128), BF16),
            vmem((1, 128), F32),
            vmem((DEVICES, 1, 128), F32),
            vmem((2, 2, 128), BF16),
            vmem((2, DEVICES, 2, 128), BF16),
            vmem((CAP, DEVICES, 8, 128), BF16),
            vmem((CAP, DEVICES, 8, 128), BF16),
            vmem((8, 128), jnp.int32),
            pltpu.SMEM((8, 128), jnp.int32),
            vmem((512, 512), BF16),
            vmem((2, 512, 512), BF16),
            vmem((2, 512, 512), BF16),
            vmem((2, 512, 512), BF16),
            dma, dma, dma, dma, dma, dma, dma((CAP,)), dma((CAP,)), dma, dma((2,)),
        ],
        compiler_params=pltpu.CompilerParams(collective_id=0, has_side_effects=True, vmem_limit_bytes=GRANT),
        name="move",
    )(factors, target)


def root_kernel(g_ref, aux_ref, first_ref, out_any, root, block, x, y, z, sems):
    copies = [pltpu.make_async_copy(first_ref, out_any.at[0], sems.at[0])]
    copies[0].start()
    works = []
    for s in range(1, CAP):
        places = (r.at[s - 1] for r in (root, block, x, y, z))
        works.append(begin(s, g_ref.at[s - 1], aux_ref, *places))
        copies.append(pltpu.make_async_copy(root.at[s - 1], out_any.at[s], sems.at[s]))
    for step in range(7):
        for s, work in enumerate(works):
            next(work, None)
            if step == 6:
                copies[s + 1].start()
    for copy in copies:
        copy.wait()


def roots(moved, aux, first):
    vmem = pltpu.VMEM
    return pl.pallas_call(
        root_kernel,
        out_shape=jax.ShapeDtypeStruct((CAP, 512, 512), F32),
        in_specs=[pl.BlockSpec(memory_space=vmem)] * 3,
        out_specs=pl.BlockSpec(memory_space=pl.ANY),
        scratch_shapes=[
            vmem((CAP - 1, 512, 512), F32),
            vmem((CAP - 1, 512, 512), BF16),
            vmem((CAP - 1, 2, 512, 512), BF16),
            vmem((CAP - 1, 2, 512, 512), BF16),
            vmem((CAP - 1, 2, 512, 512), BF16),
            pltpu.SemaphoreType.DMA((CAP,)),
        ],
        compiler_params=pltpu.CompilerParams(vmem_limit_bytes=GRANT),
        name="roots",
    )(moved, aux, first)


def shards(factors, target):
    return roots(*move(pltpu.with_memory_space_constraint(factors[0], pltpu.HBM), pltpu.with_memory_space_constraint(target.T, pltpu.HBM)))[None]


def solution(mesh):
    finer = Mesh(mesh.devices.reshape(4, 2, 4, 4), AXES)
    placed = (P(AXES, None, None, None), P(AXES, None))
    return jax.shard_map(
        shards, mesh=finer, in_specs=placed, out_specs=P(AXES, None, None, None), check_vma=False
    )
```

```python
import itertools

import jax
import jax.numpy as jnp
from jax import lax
from jax.experimental import pallas as pl
from jax.experimental.pallas import tpu as pltpu
from jax.sharding import Mesh
from jax.sharding import PartitionSpec as P

AXES = ("y", "c", "z", "x")
MESH = pl.DeviceIdType.MESH
DEVICES = 128
HALF = 256
CAP = 3
GRANT = 32 << 20
F32 = jnp.float32
BF16 = jnp.bfloat16


def iota(shape, dim):
    return lax.broadcasted_iota(jnp.int32, shape, dim)


def total(value):
    return jnp.sum(jnp.sum(value, axis=1, keepdims=True), axis=0, keepdims=True)


def step_of(digit):
    return (0x36 >> (2 * (digit & 3))) & 3


def peer(k, here):
    y, c, z, x = here
    there = (
        (y + step_of(k >> 4)) & 3,
        (c + 1 - (k >> 6)) & 1,
        (z + step_of(k >> 2)) & 3,
        (x + step_of(k)) & 3,
    )
    return there, ((there[0] * 2 + there[1]) * 4 + there[2]) * 4 + there[3]


def each_peer(here, do, start=0, stop=DEVICES - 1):
    @pl.loop(start, stop, unroll=stop - start)
    def _(k):
        do(*peer(k, here))


def pack(f_ref, t_ref, send1, facts_ref, diagonal_ref):
    row, col = iota((HALF, HALF), 0), iota((HALF, HALF), 1)
    sq = jnp.zeros((1, 1), F32)
    line = iota((2, 128), 0)
    for h in range(2):
        a = f_ref[h, 0:HALF, 0:HALF].astype(F32)
        b = f_ref[h, 0:HALF, HALF:]
        d = f_ref[h, HALF:, HALF:].astype(F32)
        bf = b.astype(F32)
        sq = sq + total(a * a + 2.0 * (bf * bf) + d * d)
        v = jnp.where(row <= col, a, d).astype(BF16)
        diagonal = jnp.sum(jnp.where(row == col, d, 0.0), axis=0, keepdims=True)
        diagonal = jnp.where(line == 0, diagonal[:, 0:128], diagonal[:, 128:])
        diagonal_ref[h] = diagonal.astype(BF16)
        for part, w in enumerate((b, v)):
            for lanes in range(2):
                start = lanes * 64 + part * 32
                piece = w[:, lanes * 128 : lanes * 128 + 128]
                send1[h, start : start + 32] = piece.reshape(32, 8, 128)
    lane = iota((1, 128), 1)
    facts = jnp.where(lane == 0, t_ref[0:1, 0:1].astype(F32), 0.0)
    facts = jnp.where(lane == 1, t_ref[0:1, 1:2].astype(F32), facts)
    facts_ref[...] = jnp.where(lane == 2, sq, facts)


def plan(me, all_facts, order, aux_ref):
    facts = all_facts[:, 0, :]
    across = facts.T
    t0, t1 = facts[:, 0:1], facts[:, 1:2]
    r0, r1, sq = across[0:1, :], across[1:2, :], across[2:3, :]
    i, j = iota((DEVICES, DEVICES), 0), iota((DEVICES, DEVICES), 1)

    def same(a, b):
        return jnp.where(a == b, 1.0, 0.0)

    def along(value):
        return jnp.sum(value, axis=1, keepdims=True)

    before = j < i
    slot0 = along(jnp.where(before, same(r0, t0) + same(r1, t0), 0.0))
    slot1 = along(jnp.where(before, same(r0, t1) + same(r1, t1), 0.0)) + same(t0, t1)
    layer = along(jnp.where((i >> 4) == (j >> 4), sq, 0.0))
    fi, fj = i.astype(F32), j.astype(F32)
    line, lane = iota((8, 128), 0), iota((8, 128), 1)
    mine = iota((1, 128), 1) == me
    wanted = jnp.zeros((8, 128), F32)
    numbers = jnp.zeros((8, 128), F32)
    for s in range(CAP):
        first = jnp.where(t0 == fj, same(slot0, s), 0.0)
        second = jnp.where(t1 == fj, same(slot1, s), 0.0)
        both = first + second
        holds = jnp.sum(first * fi + second * (fi + DEVICES), axis=0, keepdims=True)
        filled = jnp.sum(both, axis=0, keepdims=True)
        layers = jnp.sum(both * layer, axis=0, keepdims=True)
        wanted = jnp.where(line == s, holds, wanted)
        my_filled = along(jnp.where(mine, filled, 0.0))
        my_layer = along(jnp.where(mine, layers, 0.0))
        scale = 2.0 * jnp.sqrt(jnp.where(my_filled > 0, my_layer, 16384.0) / 16384.0)
        inverse = jnp.where(my_filled > 0, 1.0 / scale, 0.0)
        factor = jnp.where(my_filled > 0, lax.rsqrt(jnp.sqrt(scale)), 0.0)
        numbers = jnp.where((line == s) & (lane == 0), inverse, numbers)
        numbers = jnp.where((line == s) & (lane == 1), factor, numbers)
    order[...] = wanted.astype(jnp.int32)
    aux_ref[8:16, :] = numbers


def dot(a, b):
    return jnp.dot(a, b, preferred_element_type=F32)


LEFT, RIGHT = slice(0, HALF), slice(HALF, 2 * HALF)


def tiles(ref):
    return [ref[r, c].astype(F32) for r, c in ((LEFT, LEFT), (LEFT, RIGHT), (RIGHT, RIGHT))]


def product(*pairs):
    right = sum(dot(a[...], b[:, RIGHT]) for a, b in pairs)
    corner = sum(dot(a[LEFT, :], b[:, LEFT]) for a, b in pairs)
    return [corner, right[LEFT], right[RIGHT]]


def times(a, b):
    return product((a[0], b[0]), (a[0], b[1]), (a[1], b[0]))


def squared(a):
    high = product((a.at[0], a.at[0]))
    cross = dot(a[0], a[1])
    sides = ((LEFT, LEFT), (LEFT, RIGHT), (RIGHT, RIGHT))
    return [t + (cross[r, c] + cross[c, r].T) for t, (r, c) in zip(high, sides)]


def keep(ref, value):
    places = (LEFT, LEFT), (LEFT, RIGHT), (RIGHT, RIGHT), (RIGHT, LEFT)
    for (r, c), tile in zip(places, (*value, value[1].T)):
        high = tile.astype(BF16)
        ref[0, r, c] = high
        ref[1, r, c] = (tile - high.astype(F32)).astype(BF16)


def unfold(g, diagonal, block):
    row, col = iota((HALF, HALF), 0), iota((HALF, HALF), 1)

    def whole(part):
        return jnp.concatenate(
            [
                g[lanes * 64 + part * 32 : lanes * 64 + part * 32 + 32].reshape(HALF, 128)
                for lanes in range(2)
            ],
            axis=1,
        )

    u = whole(0)
    v = whole(1).astype(F32)
    flipped = v.T
    block[LEFT, LEFT] = jnp.where(row <= col, v, flipped).astype(BF16)
    block[LEFT, RIGHT] = u
    block[RIGHT, LEFT] = u.astype(F32).T.astype(BF16)
    corner = jnp.where(row > col, v, jnp.where(row == col, diagonal, flipped))
    block[RIGHT, RIGHT] = corner.astype(BF16)


def newton(block, inverse, factor, out, x, y, z):
    eye = jnp.where(iota((HALF, HALF), 0) == iota((HALF, HALF), 1), 1.25, 0.0)
    eyes = (eye, 0.0, eye)
    q = inverse * 0.25
    square = product((block, block))
    keep(x, [1.25 * e - (2.5 * q) * a + (s * q) * q for e, a, s in zip(eyes, tiles(block), square)])
    yield
    keep(y, squared(x))
    yield
    step = [e - t * q for e, t in zip(eyes, product((y.at[0], block), (y.at[1], block)))]
    keep(z, step)
    yield
    square = squared(z)
    keep(x, square)
    keep(y, [1.25 * t - s for t, s in zip(step, square)])
    yield
    keep(z, squared(x))
    yield
    both = [1.25 * t - f for t, f in zip(step, times(z, y))]
    keep(x, both)
    yield
    rest = product((x.at[0], block), (x.at[1], block))
    root = [(1.25 * t - r * q) * factor for t, r in zip(both, rest)]
    out[LEFT, LEFT] = root[0]
    out[LEFT, RIGHT] = root[1]
    out[RIGHT, RIGHT] = root[2]
    out[RIGHT, LEFT] = root[1].T


def begin(s, g, aux_ref, out, block, x, y, z):
    unfold(g, jnp.concatenate([aux_ref[2 * s : 2 * s + 1], aux_ref[2 * s + 1 : 2 * s + 2]], axis=1), block)
    return newton(block, aux_ref[8 + s : 9 + s, 0:1], aux_ref[8 + s : 9 + s, 1:2], out, x, y, z)


def move_kernel(
    f_hbm, t_hbm, g_ref, aux_ref, first_ref,
    t_ref, f_ref, send1, got1, facts, all_facts, diagonal, all_diagonal, send2, got2, order, order_s,
    block, x, y, z,
    facts_out, facts_in, diagonal_out, diagonal_in, out1, in1, out2, in2, local, loaded,
):
    here = tuple(lax.axis_index(a) for a in AXES)
    me = ((here[0] * 2 + here[1]) * 4 + here[2]) * 4 + here[3]
    loads = [
        pltpu.make_async_copy(f_hbm, f_ref, loaded.at[0]),
        pltpu.make_async_copy(t_hbm, t_ref, loaded.at[1]),
    ]
    for load in loads:
        load.start()
    barrier = pltpu.get_barrier_semaphore()
    each_peer(
        here,
        lambda there, _: pl.semaphore_signal(barrier, 1, device_id=there, device_id_type=MESH),
    )
    for load in loads:
        load.wait()
    pack(f_ref, t_ref, send1, facts, diagonal)
    pl.semaphore_wait(barrier, DEVICES - 1)

    def send(source, target, gone, came, *part):
        def start(there, index):
            pltpu.make_async_remote_copy(
                src_ref=source(index), dst_ref=target, send_sem=gone, recv_sem=came,
                device_id=there, device_id_type=MESH,
            ).start()

        each_peer(here, start, *part)

    def settle(buffer, *sems):
        for sem in sems:
            pltpu.make_async_copy(buffer, buffer, sem).wait()

    send(lambda index: facts, all_facts.at[me], facts_out, facts_in)
    send(lambda index: send1.at[:, index], got1.at[:, me], out1, in1)
    send(lambda index: diagonal, all_diagonal.at[:, me], diagonal_out, diagonal_in)
    all_facts[me] = facts[...]
    got1[:, me] = send1[:, me]
    all_diagonal[:, me] = diagonal[...]
    settle(all_facts.at[0 : DEVICES - 1], facts_in, facts_out)
    plan(me, all_facts, order, aux_ref)
    copy = pltpu.make_async_copy(order, order_s, local)
    copy.start()
    copy.wait()
    settle(got1.at[:, 0 : DEVICES - 1], in1, out1)

    def place(block):
        return (block >> 7) & 1, block & (DEVICES - 1)

    for s in range(CAP):

        def gather(_, index, s=s):
            send2[s, index] = got1[place(order_s[s, index])]

        bounds = (0, 32, 64, 96, DEVICES - 1) if s == 0 else (0, DEVICES - 1)
        for part in zip(bounds, bounds[1:]):
            each_peer(here, gather, *part)
            send(lambda index, s=s: send2.at[s, index], got2.at[s, me], out2.at[s], in2.at[s], *part)
        got2[s, me] = got1[place(order_s[s, me])]
    settle(all_diagonal.at[:, 0 : DEVICES - 1], diagonal_in, diagonal_out)
    for s in range(CAP):
        aux_ref[2 * s : 2 * s + 2, :] = all_diagonal[place(order_s[s, me])].astype(F32)
    settle(got2.at[0, 0 : DEVICES - 1], in2.at[0], out2.at[0])

    def store(s):
        settle(got2.at[s, 0 : DEVICES - 1], in2.at[s], out2.at[s])
        g_ref[s - 1] = got2[s]

    for step, _ in enumerate(begin(0, got2.at[0], aux_ref, first_ref, block, x, y, z)):
        if step == 5:
            store(1)
    store(2)


def move(factors, target):
    vmem, dma = pltpu.VMEM, pltpu.SemaphoreType.DMA
    return pl.pallas_call(
        move_kernel,
        out_shape=(
            jax.ShapeDtypeStruct((CAP - 1, DEVICES, 8, 128), BF16),
            jax.ShapeDtypeStruct((16, 128), F32),
            jax.ShapeDtypeStruct((512, 512), F32),
        ),
        in_specs=[pl.BlockSpec(memory_space=pltpu.HBM)] * 2,
        out_specs=[pl.BlockSpec(memory_space=vmem)] * 3,
        scratch_shapes=[
            vmem((1, 2), jnp.int32),
            vmem((2, 512, 512), BF16),
            vmem((2, DEVICES, 8, 128), BF16),
            vmem((2, DEVICES, 8, 128), BF16),
            vmem((1, 128), F32),
            vmem((DEVICES, 1, 128), F32),
            vmem((2, 2, 128), BF16),
            vmem((2, DEVICES, 2, 128), BF16),
            vmem((CAP, DEVICES, 8, 128), BF16),
            vmem((CAP, DEVICES, 8, 128), BF16),
            vmem((8, 128), jnp.int32),
            pltpu.SMEM((8, 128), jnp.int32),
            vmem((512, 512), BF16),
            vmem((2, 512, 512), BF16),
            vmem((2, 512, 512), BF16),
            vmem((2, 512, 512), BF16),
            dma, dma, dma, dma, dma, dma, dma((CAP,)), dma((CAP,)), dma, dma((2,)),
        ],
        compiler_params=pltpu.CompilerParams(collective_id=0, has_side_effects=True, vmem_limit_bytes=GRANT),
        name="move",
    )(factors, target)


def root_kernel(g_ref, aux_ref, first_ref, out_any, root, block, x, y, z, sems):
    copies = [pltpu.make_async_copy(first_ref, out_any.at[0], sems.at[0])]
    copies[0].start()
    works = []
    for s in range(1, CAP):
        places = (r.at[s - 1] for r in (root, block, x, y, z))
        works.append(begin(s, g_ref.at[s - 1], aux_ref, *places))
        copies.append(pltpu.make_async_copy(root.at[s - 1], out_any.at[s], sems.at[s]))
    for step in range(7):
        for s, work in enumerate(works):
            next(work, None)
            if step == 6:
                copies[s + 1].start()
    for copy in copies:
        copy.wait()


def roots(moved, aux, first):
    vmem = pltpu.VMEM
    return pl.pallas_call(
        root_kernel,
        out_shape=jax.ShapeDtypeStruct((CAP, 512, 512), F32),
        in_specs=[pl.BlockSpec(memory_space=vmem)] * 3,
        out_specs=pl.BlockSpec(memory_space=pl.ANY),
        scratch_shapes=[
            vmem((CAP - 1, 512, 512), F32),
            vmem((CAP - 1, 512, 512), BF16),
            vmem((CAP - 1, 2, 512, 512), BF16),
            vmem((CAP - 1, 2, 512, 512), BF16),
            vmem((CAP - 1, 2, 512, 512), BF16),
            pltpu.SemaphoreType.DMA((CAP,)),
        ],
        compiler_params=pltpu.CompilerParams(vmem_limit_bytes=GRANT),
        name="roots",
    )(moved, aux, first)


def shards(factors, target):
    return roots(*move(pltpu.with_memory_space_constraint(factors[0], pltpu.HBM), pltpu.with_memory_space_constraint(target.T, pltpu.HBM)))[None]


def solution(mesh):
    finer = Mesh(mesh.devices.reshape(4, 2, 4, 4), AXES)
    placed = (P(AXES, None, None, None), P(AXES, None))
    return jax.shard_map(
        shards, mesh=finer, in_specs=placed, out_specs=P(AXES, None, None, None), check_vma=False
    )
```
